128 devices in a mesh: fsdp: 64 (over x_lo, y, z, core), grp: 2 (over x_hi).
Axes of the slice: x: 4 (x_hi: 2, x_lo: 2; x = x_hi * 2 + x_lo), y: 4, z: 4, core: 2. Of those that a mesh axis runs over, the one named last changes fastest.
Arguments:
- hidden: bfloat16 [32768, 3072], P('fsdp', 'grp'), may hold values from -16 to 16
- queries: bfloat16 [32768, 1536], P('fsdp', 'grp'), may hold values from -6 to 6
- attn_keys: bfloat16 [32768, 1536], P('fsdp', 'grp'), may hold values from -6 to 6
- w_value: bfloat16 [1536, 3072], P('fsdp', 'grp'), may hold values from -1 to 1
- w_out: bfloat16 [1536, 3072], P('fsdp', 'grp'), may hold values from -1 to 1
- alpha: float32 [3072], P('grp'), may hold values from 0.05 to 0.5
- out_grad: bfloat16 [32768, 3072], P('fsdp', 'grp'), may hold values from -6 to 6
Outputs:
- new_hidden: bfloat16 [32768, 3072], P('fsdp', 'grp')
- grad_hidden: bfloat16 [32768, 3072], P('fsdp', 'grp')
- grad_queries: bfloat16 [32768, 1536], P('fsdp', 'grp')
- grad_keys: bfloat16 [32768, 1536], P('fsdp', 'grp')
- grad_w_value: float32 [1536, 3072], P('fsdp', 'grp')
- grad_w_out: float32 [1536, 3072], P('fsdp', 'grp')
The draws below stay inside these ranges and needn't reach their ends.
All inputs are finite; a program needn't handle non-finite values.
Results may differ from the reference program's by a relative error of at most 0.012.
The reference program's roundings to bfloat16 on the way count: a program that leaves them out, or rounds other values in their place, can miss the bound.
Values may be sent and summed in bfloat16 or wider, within the bound.
A program may use at most 192 MiB of HBM per device.

```python
import math
import jax
import jax.numpy as jnp
from jax import lax

D = 3072
HEADS = 12
HS = 128
SEQ = 512
HD = 1536
TOKENS = 32768


def column_scales(scale_key, width):
    position = jnp.arange(width, dtype=jnp.float32) / (width - 1)
    ramp_scale = jnp.exp(jnp.log(3.0) * (position - 0.5))
    roughness = jnp.exp(jax.random.uniform(scale_key, (width,), jnp.float32, -1.0, 1.0))
    return ramp_scale * roughness


def draw_hidden(key, part):
    row_key, col_key, val_key = jax.random.split(jax.random.fold_in(key, 5), 3)
    row_scale = jnp.exp(jax.random.uniform(row_key, (TOKENS, 1), jnp.float32, -1.15, 1.15))
    col_scale = column_scales(col_key, D)
    base_draw = jax.random.normal(val_key, (TOKENS, D), jnp.float32)
    return jnp.clip(base_draw * row_scale * col_scale, -16.0, 16.0).astype(jnp.bfloat16)


def weight_rows(key):
    row_key, col_key, val_key = jax.random.split(key, 3)
    row_scale = jnp.exp(jax.random.uniform(row_key, (HD, 1), jnp.float32, 0.0, jnp.log(10.0)))
    col_scale = column_scales(col_key, D)
    base_draw = jax.random.normal(val_key, (HD, D), jnp.float32)
    scaled = base_draw * row_scale * col_scale / (10.0 * D ** 0.5)
    return jnp.clip(scaled, -1.0, 1.0).astype(jnp.bfloat16)


def draw_w_value(key, part):
    return weight_rows(jax.random.fold_in(key, 11))


def draw_w_out(key, part):
    return weight_rows(jax.random.fold_in(key, 23))


def attention_pair(key):
    query_key, keys_key = jax.random.split(jax.random.fold_in(key, 37), 2)
    query_draw = jnp.clip(jax.random.normal(query_key, (TOKENS, HD), jnp.float32), -6.0, 6.0)
    keys_draw = jnp.clip(jax.random.normal(keys_key, (TOKENS, HD), jnp.float32), -6.0, 6.0)
    return (query_draw, keys_draw)


def draw_queries(key, part):
    return attention_pair(key)[0].astype(jnp.bfloat16)


def draw_attn_keys(key, part):
    return attention_pair(key)[1].astype(jnp.bfloat16)


def levels(own_key, shape, cuts, low, high):
    def one(dim, blocks):
        draws = jax.random.uniform(jax.random.fold_in(jax.random.fold_in(own_key, 6), dim), (blocks,), jnp.float32, low / len(cuts), high / len(cuts))
        return jnp.repeat(jnp.exp(draws), shape[dim] // blocks).reshape((-1,) + (1,) * (len(shape) - dim - 1))

    gain = one(*cuts[0])
    for cut in cuts[1:]:
        gain = gain * one(*cut)
    return gain


def gaussian(key, shape, scale, limit, shards=(), kind=jnp.bfloat16):
    loudness = levels(key, shape, shards, -0.22, 0.18) if shards else 1.0
    values = jax.random.normal(key, shape, jnp.float32) * scale * loudness
    return jnp.minimum(jnp.maximum(values, -limit), limit).astype(kind)


def setup_inputs(seed: int = 0) -> dict:
    seeds = jax.random.split(jax.random.key(seed), 8)
    hidden = draw_hidden(jax.random.fold_in(seeds[7], 71), 0)
    queries = draw_queries(jax.random.fold_in(seeds[7], 71), 0)
    attn_keys = draw_attn_keys(jax.random.fold_in(seeds[7], 71), 0)
    w_value = draw_w_value(jax.random.fold_in(seeds[7], 71), 0)
    w_out = draw_w_out(jax.random.fold_in(seeds[7], 71), 0)
    alpha = jnp.clip(jnp.exp(math.log(0.5) - 2.3025851 * jax.random.uniform(seeds[5], (D,), jnp.float32) ** levels(seeds[5], (D,), ((0, 2),), -0.2, 0.2)), 0.05, 0.5)
    out_grad = gaussian(seeds[6], (TOKENS, D), 1.0, 6.0, ((0, 64), (1, 2)))
    return dict(hidden=hidden, queries=queries, attn_keys=attn_keys, w_value=w_value, w_out=w_out, alpha=alpha, out_grad=out_grad)


EPS = 1e-06

def contract_last(left, right):
    return lax.dot_general(left, right, (((1,), (1,)), ((), ())), preferred_element_type=jnp.float32)

def contract_first(left, right):
    return lax.dot_general(left, right, (((0,), (0,)), ((), ())), preferred_element_type=jnp.float32)

def causal_probs(query_head, key_head):
    length = query_head.shape[0]
    score_scale = query_head.shape[1] ** (-0.5)
    scores = contract_last(query_head, key_head) * score_scale
    row_pos = lax.broadcasted_iota(jnp.int32, (length, length), 0)
    col_pos = lax.broadcasted_iota(jnp.int32, (length, length), 1)
    scores = jnp.where(row_pos >= col_pos, scores, -1e+30)
    row_peak = lax.optimization_barrier(jnp.max(scores, axis=1, keepdims=True))
    exp_terms = jnp.exp(scores - row_peak)
    return exp_terms / lax.optimization_barrier(jnp.sum(exp_terms, axis=1, keepdims=True))

def head_forward(items):
    query_head, key_head, value_head = items
    attn_prob = causal_probs(query_head, key_head)
    return jnp.dot(attn_prob.astype(jnp.bfloat16), value_head, preferred_element_type=jnp.float32).astype(jnp.bfloat16)

def head_backward(items):
    query_head, key_head, value_head, grad_head = items
    score_scale = query_head.shape[1] ** (-0.5)
    attn_prob = causal_probs(query_head, key_head)
    prob_half = attn_prob.astype(jnp.bfloat16)
    grad_prob = contract_last(grad_head, value_head)
    row_delta = lax.optimization_barrier(jnp.sum(attn_prob * grad_prob, axis=1, keepdims=True))
    grad_score = (attn_prob * (grad_prob - row_delta)).astype(jnp.bfloat16)
    grad_query = (jnp.dot(grad_score, key_head, preferred_element_type=jnp.float32) * score_scale).astype(jnp.bfloat16)
    grad_key = (contract_first(grad_score, query_head) * score_scale).astype(jnp.bfloat16)
    grad_value = contract_first(prob_half, grad_head).astype(jnp.bfloat16)
    return (grad_query, grad_key, grad_value)

def to_heads(block):
    return block.reshape(TOKENS // SEQ, SEQ, HEADS, HS).transpose(0, 2, 1, 3).reshape(-1, SEQ, HS)

def from_heads(stacked):
    return stacked.reshape(TOKENS // SEQ, HEADS, SEQ, HS).transpose(0, 2, 1, 3).reshape(TOKENS, HEADS * HS)

def unit_rows(weights):
    weights_f = weights.astype(jnp.float32)
    norms = jnp.sqrt(lax.optimization_barrier(jnp.sum(weights_f * weights_f, axis=1, keepdims=True)) + EPS)
    return (weights_f / norms, norms)

def unit_back(grad_unit, unit, norms):
    row_dot = lax.optimization_barrier(jnp.sum(grad_unit * unit, axis=1, keepdims=True))
    return (grad_unit - unit * row_dot) / norms

def reference(hidden, queries, attn_keys, w_value, w_out, alpha, out_grad):
    unit_v, norm_v = unit_rows(w_value)
    unit_o, norm_o = unit_rows(w_out)
    weight_v = unit_v.astype(jnp.bfloat16)
    weight_o = unit_o.astype(jnp.bfloat16)
    values = contract_last(hidden, weight_v).astype(jnp.bfloat16)
    q_heads = to_heads(queries)
    k_heads = to_heads(attn_keys)
    v_heads = to_heads(values)
    attn = from_heads(lax.map(head_forward, (q_heads, k_heads, v_heads)))
    proj = jnp.dot(attn, weight_o, preferred_element_type=jnp.float32)
    hidden_f = hidden.astype(jnp.float32)
    proj_rs = lax.rsqrt(lax.optimization_barrier(jnp.mean(proj * proj, axis=1, keepdims=True)) + EPS)
    mixed = hidden_f + alpha * (proj * proj_rs - hidden_f)
    mix_rs = lax.rsqrt(lax.optimization_barrier(jnp.mean(mixed * mixed, axis=1, keepdims=True)) + EPS)
    new_hidden = (mixed * mix_rs).astype(jnp.bfloat16)
    grad_out = out_grad.astype(jnp.float32)
    grad_mix = mix_rs * (grad_out - mixed * mix_rs * mix_rs * lax.optimization_barrier(jnp.mean(grad_out * mixed, axis=1, keepdims=True)))
    grad_res = grad_mix * (1.0 - alpha)
    grad_pn = grad_mix * alpha
    grad_proj = proj_rs * (grad_pn - proj * proj_rs * proj_rs * lax.optimization_barrier(jnp.mean(grad_pn * proj, axis=1, keepdims=True)))
    grad_proj_b = grad_proj.astype(jnp.bfloat16)
    grad_attn = contract_last(grad_proj_b, weight_o).astype(jnp.bfloat16)
    gw_o = contract_first(attn, grad_proj_b)
    grad_q, grad_k, grad_v = lax.map(head_backward, (q_heads, k_heads, v_heads, to_heads(grad_attn)))
    grad_values = from_heads(grad_v)
    grad_hidden = (grad_res + jnp.dot(grad_values, weight_v, preferred_element_type=jnp.float32)).astype(jnp.bfloat16)
    gw_v = contract_first(grad_values, hidden)
    grad_w_value = unit_back(gw_v, unit_v, norm_v)
    grad_w_out = unit_back(gw_o, unit_o, norm_o)
    return (new_hidden, grad_hidden, from_heads(grad_q), from_heads(grad_k), grad_w_value, grad_w_out)
```

```python
import jax
import jax.numpy as jnp
from jax import lax
from jax.experimental import pallas as pl
from jax.experimental.pallas import tpu as pltpu
from jax.sharding import Mesh
from jax.sharding import PartitionSpec as P

D = 3072
EPS = 1e-06
AXES = ("fsdp_0", "fsdp_1", "fsdp_2", "fsdp_3", "grp")
FSDP = AXES[:4]
SCALE = 128 ** (-0.5)
F32 = jnp.float32
BF16 = jnp.bfloat16
MESH = pl.DeviceIdType.MESH


def nt(a, b):
    return lax.dot_general(a, b, (((1,), (1,)), ((), ())), preferred_element_type=F32)


def tn(a, b):
    return lax.dot_general(a, b, (((0,), (0,)), ((), ())), preferred_element_type=F32)


def nn(a, b):
    return lax.dot_general(a, b, (((1,), (0,)), ((), ())), preferred_element_type=F32)


def lanes(start, size):
    return pl.ds(pl.multiple_of(start, 128), size)


def kernel(
    hid_h, q_h, k_h, wv_h, wo_h, al, og_h,
    nh_h, gh_h, gq_h, gk_h, gwv_h, gwo_h,
    hid, q, k, og, wraw, unit, nrm, nsend, nrecv, usr, W,
    vsend, vrecv, vown, V, Pr, ATT, proj, gpb, mom, msend, mrecv,
    garecv, GA, gsb, gq, gk, GV, gss, gsr, RSA, r1b, S1, r2b, xk, xs, xr, fin, gown, rds, rdr,
    in_m, out_m, nm_s, nm_r, us_s, us_r, ax_s, ax_r, p1_s, p1_r, p2_s, p2_r, sb_s, sb_r,
    ex_s, ex_r, gs_s, gs_r, r1_s, r1_r, r2_s, r2_r, rx_s, rx_r, fd_s, fd_r,
):
    x, y, z, c, g = (lax.axis_index(a) for a in AXES)
    oc = 1 - c
    og_ = 1 - g

    def ring(v, d):
        return lax.rem(v + d, 4)

    sib = (x, y, z, oc, g)
    mate = (x, y, z, c, og_)
    xdev = (1 - x, y, z, c, g)

    def ydev(d):
        return (x, ring(y, d), z, c, g)

    def zdev(d):
        return (x, y, ring(z, d), c, g)

    def rc(src, dst, ss, rs, dev):
        return pltpu.make_async_remote_copy(
            src_ref=src, dst_ref=dst, send_sem=ss, recv_sem=rs, device_id=dev, device_id_type=MESH
        )

    ins = [
        pltpu.make_async_copy(wv_h, wraw.at[0], in_m.at[0]),
        pltpu.make_async_copy(wo_h, wraw.at[1], in_m.at[1]),
        pltpu.make_async_copy(q_h, q, in_m.at[2]),
        pltpu.make_async_copy(k_h, k, in_m.at[3]),
        pltpu.make_async_copy(hid_h, hid, in_m.at[4]),
        pltpu.make_async_copy(og_h, og, in_m.at[5]),
    ]
    for cp in ins:
        cp.start()

    barrier = pltpu.get_barrier_semaphore()
    peers = [sib, mate, xdev] + [ydev(d) for d in (1, 2, 3)] + [zdev(d) for d in (1, 2, 3)]
    for dev in peers:
        pl.semaphore_signal(barrier, inc=1, device_id=dev, device_id_type=MESH)

    gsb[...] = jnp.zeros_like(gsb)
    ins[0].wait()
    ins[1].wait()
    for w in range(2):
        rows = wraw[w].astype(F32)
        nsend[w] = jnp.broadcast_to(jnp.sum(rows * rows, axis=1, keepdims=True), (24, 128))
    pl.semaphore_wait(barrier, len(peers))
    ncp = rc(nsend, nrecv, nm_s.at[0], nm_r.at[0], mate)
    ncp.start()

    def probs(first, last):
        def one(h, carry):
            hc = lanes(128 * h, 128)
            for r in range(4):
                n = 128 * (r + 1)
                rr = pl.ds(128 * r, 128)
                s = nt(q[rr, hc], k[pl.ds(0, n), hc]) * SCALE
                row = lax.broadcasted_iota(jnp.int32, (128, n), 0) + 128 * r
                col = lax.broadcasted_iota(jnp.int32, (128, n), 1)
                s = jnp.where(row >= col, s, -1e30)
                e = jnp.exp(s - jnp.max(s, axis=1, keepdims=True))
                Pr[h, rr, pl.ds(0, n)] = e / jnp.sum(e, axis=1, keepdims=True)
                if r < 3:
                    Pr[h, rr, pl.ds(n, 512 - n)] = jnp.zeros((128, 512 - n), F32)
            return carry

        lax.fori_loop(first, last, one, 0)

    ins[2].wait()
    ins[3].wait()
    probs(0, 1)

    ncp.wait()
    for w in range(2):
        norm = jnp.sqrt(nsend[w] + nrecv[w] + EPS)
        nrm[w] = norm
        unit[w] = wraw[w].astype(F32) / norm[:, :1]
    ucp = rc(unit.at[:, :, lanes(768 * oc, 768)], usr, us_s.at[0], us_r.at[0], sib)
    ucp.start()
    ucp.wait()
    for w in range(2):
        mine = unit[w, :, lanes(768 * c, 768)]
        other = usr[w]
        low = jnp.where(c == 0, mine, other)
        high = jnp.where(c == 0, other, mine)
        W[w, x, y, z, :, lanes(768 * c, 768)] = jnp.concatenate([low, high], axis=0).astype(BF16)

    def cols(s):
        return lanes(768 * c + 384 * s, 384)

    axs = []
    for w in range(2):
        blk = W.at[w, x, y, z, :, lanes(768 * c, 768)]
        axs.append(rc(blk, blk, ax_s.at[w], ax_r.at[w], xdev))
    p1 = {}
    p2 = {}
    sbc = {}
    for w in range(2):
        for s in range(2):
            for d in (1, 2, 3):
                blk = W.at[w, :, y, z, :, cols(s)]
                p1[w, s, d] = rc(
                    blk, blk, p1_s.at[w, s, d - 1], p1_r.at[w, s, d - 1], ydev(d) if s == 0 else zdev(d)
                )
                for e in range(4):
                    if s == 0:
                        blk = W.at[w, :, ring(y, 4 - e), z, :, cols(s)]
                        dev = zdev(d)
                    else:
                        blk = W.at[w, :, y, ring(z, 4 - e), :, cols(s)]
                        dev = ydev(d)
                    p2[w, s, e, d] = rc(blk, blk, p2_s.at[w, s, e, d - 1], p2_r.at[w, s, e, d - 1], dev)
            for e in range(4):
                if s == 0:
                    blk = W.at[w, :, :, ring(z, 4 - e), :, cols(s)]
                else:
                    blk = W.at[w, :, ring(y, 4 - e), :, :, cols(s)]
                sbc[w, s, e] = rc(blk, blk, sb_s.at[w, s, e], sb_r.at[w, s, e], sib)

    def gather_first(w):
        axs[w].wait()
        for d in (1, 2, 3):
            for s in range(2):
                p1[w, s, d].start()
        for d in (1, 2, 3):
            for s in range(2):
                p2[w, s, 0, d].start()

    def gather_second(w):
        for d in (1, 2, 3):
            for s in range(2):
                p1[w, s, d].wait()
                for e in (1, 2, 3):
                    p2[w, s, d, e].start()
        for s in range(2):
            sbc[w, s, 0].start()

    def gather_last(w):
        for d in (1, 2, 3):
            for s in range(2):
                for e in range(4):
                    p2[w, s, e, d].wait()
                sbc[w, s, d].start()
        for s in range(2):
            for e in range(4):
                sbc[w, s, e].wait()

    axs[0].start()
    axs[1].start()
    probs(1, 2)
    gather_first(0)
    probs(2, 3)
    gather_second(0)
    gather_first(1)
    probs(3, 6)
    ins[4].wait()
    gather_last(0)

    exs = {}

    def exchange(kind, j, src, dst):
        cp = rc(src, dst, ex_s.at[kind, j], ex_r.at[kind, j], mate)
        cp.start()
        exs[kind, j] = cp

    for j in range(2):
        part = nt(hid[...], W[0, og_, 2 * j : 2 * j + 2].reshape(384, 1536))
        vsend[j] = part.astype(BF16)
        exchange(0, j, vsend.at[j], vrecv.at[j])
    for j in range(2):
        vown[j] = nt(hid[...], W[0, g, 2 * j : 2 * j + 2].reshape(384, 1536))
    gather_second(1)
    for j in range(2):
        exs[0, j].wait()
        V[j] = (vown[j] + vrecv[j].astype(F32)).astype(BF16)

        def fwd(i, carry):
            hc = lanes(128 * i, 128)
            vals = V[j, :, hc]
            ATT[:, lanes(768 * g + 384 * j + 128 * i, 128)] = nn(
                Pr[3 * j + i].astype(BF16), vals
            ).astype(BF16)
            return carry

        lax.fori_loop(0, 3, fwd, 0)
        blk = ATT.at[:, lanes(768 * g + 384 * j, 384)]
        exchange(1, j, blk, blk)
    gather_last(1)

    def proj_own(n, carry):
        nc = lanes(384 * n, 384)
        proj[:, nc] = nn(ATT[:, lanes(768 * g, 768)], W[1, g, :, :, :, nc].reshape(768, 384))
        return carry

    lax.fori_loop(0, 4, proj_own, 0)
    for j in range(2):
        exs[1, j].wait()

        def proj_more(n, carry):
            nc = lanes(384 * n, 384)
            proj[:, nc] += nn(
                ATT[:, lanes(768 * og_ + 384 * j, 384)],
                W[1, og_, 2 * j : 2 * j + 2, :, :, nc].reshape(384, 384),
            )
            return carry

        lax.fori_loop(0, 4, proj_more, 0)

    ins[5].wait()
    lane = lax.broadcasted_iota(jnp.int32, (16, 128), 1)

    def sums(i, carry):
        rr = pl.ds(pl.multiple_of(16 * i, 16), 16)
        a = al[...]
        kr = 1.0 - a
        p = proj[rr, :]
        hf = hid[rr, :].astype(F32)
        go = og[rr, :].astype(F32)
        kh = kr * hf
        ap = a * p
        parts = (p * p, kh * kh, kh * ap, ap * ap, go * kh, go * ap)
        acc = jnp.zeros((16, 128), F32)
        for j, v in enumerate(parts):
            acc = jnp.where(lane == j, jnp.sum(v, axis=1, keepdims=True), acc)
        mom[rr, :] = acc
        return carry

    lax.fori_loop(0, 32, sums, 0)
    msend[...] = mom[...].T[:8]
    mcp = rc(msend, mrecv.at[pl.ds(0, 8)], nm_s.at[1], nm_r.at[1], mate)
    mrecv[pl.ds(8, 120), :] = jnp.zeros((120, 512), F32)
    mcp.start()
    mcp.wait()
    mom[...] = mom[...] + mrecv[...].T

    def apply(i, carry):
        rr = pl.ds(pl.multiple_of(16 * i, 16), 16)
        a = al[...]
        kr = 1.0 - a
        m = mom[rr, :]
        p = proj[rr, :]
        hf = hid[rr, :].astype(F32)
        go = og[rr, :].astype(F32)
        pr = lax.rsqrt(m[:, 0:1] / D + EPS)
        mm = (m[:, 1:2] + 2.0 * pr * m[:, 2:3] + pr * pr * m[:, 3:4]) / D
        mr = lax.rsqrt(mm + EPS)
        gm = (m[:, 4:5] + pr * m[:, 5:6]) / D
        pm = (mr * m[:, 5:6] - mr * mr * mr * gm * (m[:, 2:3] + pr * m[:, 3:4])) / D
        mixed = hf + a * (p * pr - hf)
        og[rr, :] = (mixed * mr).astype(BF16)
        gmix = mr * (go - mixed * (mr * mr * gm))
        proj[rr, :] = gmix * kr
        gpb[rr, :] = (pr * (gmix * a - p * (pr * pr * pm))).astype(BF16)
        return carry

    lax.fori_loop(0, 32, apply, 0)
    outs = [pltpu.make_async_copy(og, nh_h, out_m.at[0])]
    outs[0].start()

    for j in range(2):
        vsend[j] = nt(gpb[...], W[1, og_, 2 * j : 2 * j + 2].reshape(384, 1536)).astype(BF16)
        exchange(2, j, vsend.at[j], garecv.at[j])

    gsc = {}
    r1c = {}
    r2c = {}

    def half(p):
        return g if p == 0 else og_

    def rs_partner(w, p, left, right):
        for j in range(2):
            gss[p, pl.ds(384 * j, 384), :] = tn(
                left[:, lanes(768 * half(p) + 384 * j, 384)], right[:, lanes(768 * oc, 768)]
            ).astype(BF16)
            rr = pl.ds(384 * j, 384)
            gsc[w, p, j] = rc(
                gss.at[p, rr], gsr.at[w, p, rr], gs_s.at[w, p, j], gs_r.at[w, p, j], sib
            )
            gsc[w, p, j].start()

    def rs_own(w, p, left, right):
        for j in range(2):
            part = tn(left[:, lanes(768 * half(p) + 384 * j, 384)], right[:, lanes(768 * c, 768)])
            gsc[w, p, j].wait()
            total = part + gsr[w, p, pl.ds(384 * j, 384), :].astype(F32)
            RSA[p, 2 * j : 2 * j + 2] = total.astype(BF16).reshape(2, 4, 48, 768)
        for d in (1, 2, 3):
            r1c[w, p, 0, d] = rc(
                RSA.at[p, :, ring(z, d), :, pl.ds(0, 384)], r1b.at[w, p, 0, d - 1],
                r1_s.at[w, p, 0, d - 1], r1_r.at[w, p, 0, d - 1], zdev(d),
            )
            r1c[w, p, 0, d].start()
            r1c[w, p, 1, d] = rc(
                RSA.at[p, ring(y, d), :, :, pl.ds(384, 384)], r1b.at[w, p, 1, d - 1],
                r1_s.at[w, p, 1, d - 1], r1_r.at[w, p, 1, d - 1], ydev(d),
            )
            r1c[w, p, 1, d].start()

    def rs_second(w, p):
        for s in range(2):
            for d in (1, 2, 3):
                r1c[w, p, s, d].wait()
            for b in range(4):
                if s == 0:
                    acc = RSA[p, b, z, :, pl.ds(0, 384)].astype(F32)
                else:
                    acc = RSA[p, y, b, :, pl.ds(384, 384)].astype(F32)
                for d in range(3):
                    acc += r1b[w, p, s, d, b].astype(F32)
                S1[p, s, b] = acc.astype(BF16)
            for d in (1, 2, 3):
                at = ring(y, d) if s == 0 else ring(z, d)
                dev = ydev(d) if s == 0 else zdev(d)
                r2c[w, p, s, d] = rc(
                    S1.at[p, s, at], r2b.at[w, p, s, d - 1],
                    r2_s.at[w, p, s, d - 1], r2_r.at[w, p, s, d - 1], dev,
                )
                r2c[w, p, s, d].start()

    def rs_third(w, p):
        for s in range(2):
            for d in (1, 2, 3):
                r2c[w, p, s, d].wait()
            acc = S1[p, s, y if s == 0 else z].astype(F32)
            for d in range(3):
                acc += r2b[w, p, s, d].astype(F32)
            xk[w, p, :, pl.ds(384 * s, 384)] = acc
            xs[w, p, :, pl.ds(384 * s, 384)] = acc.astype(BF16)

    away = jnp.where(x == g, 1, 0)
    rxc = [rc(xs.at[w, away], xr.at[w], rx_s.at[w], rx_r.at[w], xdev) for w in range(2)]
    fdc = [
        rc(
            fin.at[w, pl.ds(pl.multiple_of(24 * oc, 8), 24)], gown.at[w, :, lanes(768 * c, 768)],
            fd_s.at[w], fd_r.at[w], sib,
        )
        for w in range(2)
    ]

    def rs_owner(w):
        rxc[w].wait()
        fin[w] = xk[w, 1 - away] + xr[w].astype(F32)
        gown[w, :, lanes(768 * c, 768)] = fin[w, pl.ds(pl.multiple_of(24 * c, 8), 24), :]
        fdc[w].start()

    rs_partner(1, 0, ATT, gpb)
    rs_partner(1, 1, ATT, gpb)
    for j in range(2):
        vown[j] = nt(gpb[...], W[1, g, 2 * j : 2 * j + 2].reshape(384, 1536))
    rs_own(1, 0, ATT, gpb)
    rs_own(1, 1, ATT, gpb)

    for j in range(2):
        exs[2, j].wait()
        GA[...] = (vown[j] + garecv[j].astype(F32)).astype(BF16)

        def bwd(i, carry):
            h = 3 * j + i
            hc = lanes(128 * h, 128)
            ic = lanes(128 * i, 128)
            for r in range(4):
                n = 128 * (r + 1)
                rr = pl.ds(128 * r, 128)
                gp = nt(GA[rr, ic], V[j, pl.ds(0, n), ic])
                pb = Pr[h, rr, pl.ds(0, n)]
                delta = jnp.sum(pb * gp, axis=1, keepdims=True)
                gs = (pb * (gp - delta)).astype(BF16)
                gsb[rr, pl.ds(0, n)] = gs
                gq[rr, hc] = (nn(gs, k[pl.ds(0, n), hc]) * SCALE).astype(BF16)
            gk[:, hc] = (tn(gsb[...], q[:, hc]) * SCALE).astype(BF16)
            GV[:, lanes(768 * g + 384 * j + 128 * i, 128)] = tn(
                Pr[h].astype(BF16), GA[:, ic]
            ).astype(BF16)
            return carry

        lax.fori_loop(0, 3, bwd, 0)
        blk = GV.at[:, lanes(768 * g + 384 * j, 384)]
        exchange(3, j, blk, blk)
        if j == 0:
            rs_second(1, 0)
            rs_second(1, 1)
    outs.append(pltpu.make_async_copy(gq, gq_h, out_m.at[1]))
    outs.append(pltpu.make_async_copy(gk, gk_h, out_m.at[2]))
    outs[1].start()
    outs[2].start()
    rs_third(1, 0)
    rs_third(1, 1)
    rxc[1].start()

    rs_partner(0, 0, GV, hid)
    rs_own(0, 0, GV, hid)
    rs_owner(1)
    exs[3, 0].wait()
    exs[3, 1].wait()
    rs_partner(0, 1, GV, hid)
    rs_own(0, 1, GV, hid)
    rs_second(0, 0)

    def hidden_grad(n, carry):
        nc = lanes(384 * n, 384)
        gpb[:, nc] = (proj[:, nc] + nn(GV[...], W[0, :, :, :, :, nc].reshape(1536, 384))).astype(BF16)
        return carry

    lax.fori_loop(0, 2, hidden_grad, 0)
    rs_second(0, 1)
    rs_third(0, 0)
    lax.fori_loop(2, 4, hidden_grad, 0)
    outs.append(pltpu.make_async_copy(gpb, gh_h, out_m.at[3]))
    outs[3].start()
    rs_third(0, 1)
    rxc[0].start()
    rs_owner(0)
    fdc[0].wait()
    fdc[1].wait()
    for w in range(2):
        rds[w] = jnp.broadcast_to(jnp.sum(gown[w] * unit[w], axis=1, keepdims=True), (24, 128))
    rcp = rc(rds, rdr, nm_s.at[2], nm_r.at[2], mate)
    rcp.start()
    rcp.wait()
    for w in range(2):
        dot = (rds[w] + rdr[w])[:, :1]
        gown[w] = (gown[w] - unit[w] * dot) / nrm[w][:, :1]
    outs.append(pltpu.make_async_copy(gown.at[0], gwv_h, out_m.at[4]))
    outs.append(pltpu.make_async_copy(gown.at[1], gwo_h, out_m.at[5]))
    outs[4].start()
    outs[5].start()
    for cp in outs:
        cp.wait()


def shards(hidden, queries, attn_keys, w_value, w_out, alpha, out_grad):
    vm = pltpu.VMEM
    dma = pltpu.SemaphoreType.DMA
    hbm = pl.BlockSpec(memory_space=pltpu.HBM)
    scratch = [
        vm((512, 1536), BF16), vm((512, 768), BF16), vm((512, 768), BF16), vm((512, 1536), BF16),
        vm((2, 24, 1536), BF16), vm((2, 24, 1536), F32), vm((2, 24, 128), F32),
        vm((2, 24, 128), F32), vm((2, 24, 128), F32), vm((2, 24, 768), F32),
        vm((2, 2, 4, 4, 48, 1536), BF16),
        vm((2, 512, 384), BF16), vm((2, 512, 384), BF16), vm((2, 512, 384), F32), vm((2, 512, 384), BF16),
        vm((6, 512, 512), F32), vm((512, 1536), BF16), vm((512, 1536), F32), vm((512, 1536), BF16),
        vm((512, 128), F32), vm((8, 512), F32), vm((128, 512), F32),
        vm((2, 512, 384), BF16), vm((512, 384), BF16), vm((512, 512), BF16),
        vm((512, 768), BF16), vm((512, 768), BF16), vm((512, 1536), BF16),
        vm((2, 768, 768), BF16), vm((2, 2, 768, 768), BF16), vm((2, 4, 4, 48, 768), BF16),
        vm((2, 2, 2, 3, 4, 48, 384), BF16), vm((2, 2, 4, 48, 384), BF16), vm((2, 2, 2, 3, 48, 384), BF16),
        vm((2, 2, 48, 768), F32), vm((2, 2, 48, 768), BF16), vm((2, 48, 768), BF16),
        vm((2, 48, 768), F32), vm((2, 24, 1536), F32), vm((2, 24, 128), F32), vm((2, 24, 128), F32),
        dma((6,)), dma((6,)), dma((3,)), dma((3,)), dma((1,)), dma((1,)), dma((2,)), dma((2,)),
        dma((2, 2, 3)), dma((2, 2, 3)), dma((2, 2, 4, 3)), dma((2, 2, 4, 3)), dma((2, 2, 4)), dma((2, 2, 4)),
        dma((4, 2)), dma((4, 2)), dma((2, 2, 2)), dma((2, 2, 2)),
        dma((2, 2, 2, 3)), dma((2, 2, 2, 3)), dma((2, 2, 2, 3)), dma((2, 2, 2, 3)),
        dma((2,)), dma((2,)), dma((2,)), dma((2,)),
    ]
    sds = jax.ShapeDtypeStruct
    return pl.pallas_call(
        kernel,
        out_shape=(
            sds((512, 1536), BF16), sds((512, 1536), BF16), sds((512, 768), BF16),
            sds((512, 768), BF16), sds((24, 1536), F32), sds((24, 1536), F32),
        ),
        in_specs=[hbm] * 5 + [pl.BlockSpec(memory_space=pltpu.VMEM), hbm],
        out_specs=[hbm] * 6,
        scratch_shapes=scratch,
        compiler_params=pltpu.CompilerParams(
            collective_id=0, has_side_effects=True, vmem_limit_bytes=67043328
        ),
        name="sublayer",
    )(hidden, queries, attn_keys, w_value, w_out, alpha.reshape(1, 1536), out_grad)


def solution(mesh):
    torus = Mesh(mesh.devices.reshape(2, 4, 4, 2, mesh.shape["grp"]), AXES)
    both = P(FSDP, "grp")
    return jax.shard_map(
        shards,
        mesh=torus,
        in_specs=(both, both, both, both, both, P("grp"), both),
        out_specs=(both,) * 6,
        check_vma=False,
    )
```

```python
import jax
import jax.numpy as jnp
from jax import lax
from jax.experimental import pallas as pl
from jax.experimental.pallas import tpu as pltpu
from jax.sharding import Mesh
from jax.sharding import PartitionSpec as P

D = 3072
EPS = 1e-06
AXES = ("fsdp_0", "fsdp_1", "fsdp_2", "fsdp_3", "grp")
FSDP = AXES[:4]
SCALE = 128 ** (-0.5)
F32 = jnp.float32
BF16 = jnp.bfloat16
MESH = pl.DeviceIdType.MESH


def nt(a, b):
    return lax.dot_general(a, b, (((1,), (1,)), ((), ())), preferred_element_type=F32)


def tn(a, b):
    return lax.dot_general(a, b, (((0,), (0,)), ((), ())), preferred_element_type=F32)


def nn(a, b):
    return lax.dot_general(a, b, (((1,), (0,)), ((), ())), preferred_element_type=F32)


def lanes(start, size):
    return pl.ds(pl.multiple_of(start, 128), size)


def kernel(
    hid_h, q_h, k_h, wv_h, wo_h, al, og_h,
    nh_h, gh_h, gq_h, gk_h, gwv_h, gwo_h,
    hid, q, k, og, wraw, unit, nrm, nsend, nrecv, rawr, U48, W,
    vsend, vrecv, vown, V, Pr, ATT, proj, gpb, mom, msend, mrecv,
    gasend, garecv, GA, gsb, gq, gk, GV, gss, gsr, RSA, r1b, S1, r2b, xk, xs, xr, gpt, gown, rds, rdr,
    in_m, out_m, nm_s, nm_r, us_s, us_r, p1_s, p1_r, p2_s, p2_r, sb_s, sb_r,
    ex_s, ex_r, gs_s, gs_r, r1_s, r1_r, r2_s, r2_r, fd_s, fd_r,
):
    x, y, z, c, g = (lax.axis_index(a) for a in AXES)
    oc = 1 - c
    og_ = 1 - g

    def ring(v, d):
        return lax.rem(v + d, 4)

    def row(i):
        return (1 - x if i & 4 else x, y, z, oc if i & 2 else c, og_ if i & 1 else g)

    mate = row(1)
    sib = row(2)

    def ydev(d):
        return (x, ring(y, d), z, c, g)

    def zdev(d):
        return (x, y, ring(z, d), c, g)

    def rc(src, dst, ss, rs, dev):
        return pltpu.make_async_remote_copy(
            src_ref=src, dst_ref=dst, send_sem=ss, recv_sem=rs, device_id=dev, device_id_type=MESH
        )

    ins = [
        pltpu.make_async_copy(wv_h, wraw.at[0], in_m.at[0]),
        pltpu.make_async_copy(wo_h, wraw.at[1], in_m.at[1]),
        pltpu.make_async_copy(q_h, q, in_m.at[2]),
        pltpu.make_async_copy(k_h, k, in_m.at[3]),
        pltpu.make_async_copy(hid_h, hid, in_m.at[4]),
        pltpu.make_async_copy(og_h, og, in_m.at[5]),
    ]
    for cp in ins:
        cp.start()

    barrier = pltpu.get_barrier_semaphore()
    peers = [row(i) for i in range(1, 8)] + [ydev(d) for d in (1, 2, 3)] + [zdev(d) for d in (1, 2, 3)]
    for dev in peers:
        pl.semaphore_signal(barrier, inc=1, device_id=dev, device_id_type=MESH)

    gsb[...] = jnp.zeros_like(gsb)
    ins[0].wait()
    ins[1].wait()
    lane24 = lax.broadcasted_iota(jnp.int32, (24, 128), 1)
    sq = [jnp.sum(wraw[w].astype(F32) * wraw[w].astype(F32), axis=1, keepdims=True) for w in range(2)]
    nsend[...] = jnp.where(lane24 == 0, sq[0], sq[1])
    pl.semaphore_wait(barrier, len(peers))
    for i in range(1, 8):
        rc(nsend, nrecv.at[i - 1], nm_s.at[0], nm_r.at[0], row(i)).start()
    for w in range(2):
        for j, i in enumerate((2, 4, 6)):
            rc(
                wraw.at[w, :, lanes(768 * (oc if i & 2 else c), 768)], rawr.at[w, j],
                us_s.at[w], us_r.at[w], row(i),
            ).start()

    def probs(first, last):
        def one(h, carry):
            hc = lanes(128 * h, 128)
            for r in range(4):
                n = 128 * (r + 1)
                rr = pl.ds(128 * r, 128)
                s = nt(q[rr, hc], k[pl.ds(0, n), hc]) * SCALE
                row_at = lax.broadcasted_iota(jnp.int32, (128, n), 0) + 128 * r
                col_at = lax.broadcasted_iota(jnp.int32, (128, n), 1)
                s = jnp.where(row_at >= col_at, s, -1e30)
                e = jnp.exp(s - jnp.max(s, axis=1, keepdims=True))
                Pr[h, rr, pl.ds(0, n)] = e / jnp.sum(e, axis=1, keepdims=True)
                if r < 3:
                    Pr[h, rr, pl.ds(n, 512 - n)] = jnp.zeros((128, 512 - n), F32)
            return carry

        lax.fori_loop(first, last, one, 0)

    ins[2].wait()
    ins[3].wait()
    probs(0, 1)

    rc(nrecv, nrecv, nm_s.at[0], nm_r.at[0], sib).wait()
    sq = [nsend[...]] + [nrecv[i] for i in range(7)]
    norms = [jnp.sqrt(sq[2 * i] + sq[2 * i + 1] + EPS) for i in range(4)]
    nrm[...] = norms[0]

    def unit_rows(w):
        rc(rawr.at[w], rawr.at[w], us_s.at[w], us_r.at[w], sib).wait()
        div = [norms[i][:, w : w + 1] for i in range(4)]
        unit[w] = wraw[w].astype(F32) / div[0]
        near = (unit[w, :, lanes(768 * c, 768)], rawr[w, 0].astype(F32) / div[1])
        far = (rawr[w, 1].astype(F32) / div[2], rawr[w, 2].astype(F32) / div[3])
        for i, (mine, other) in enumerate((near, far)):
            low = jnp.where(c == 0, mine, other)
            high = jnp.where(c == 0, other, mine)
            block = jnp.concatenate([low, high], axis=0)
            U48[w, i] = block
            W[w, 1 - x if i else x, y, z, :, lanes(768 * c, 768)] = block.astype(BF16)

    unit_rows(0)

    def cols(s):
        return lanes(768 * c + 384 * s, 384)

    def own_block(w, f, s):
        return W.at[w, g if f else og_, y, z, :, cols(s)]

    def plane(w, f, s, e):
        if s == 0:
            return W.at[w, g if f else og_, :, ring(z, 4 - e), :, cols(s)]
        return W.at[w, g if f else og_, ring(y, 4 - e), :, :, cols(s)]

    def ring_dev(s, first, d):
        return ydev(d) if (s == 0) == first else zdev(d)

    def first_copy(w, f, s, d):
        blk = own_block(w, f, s)
        return rc(blk, blk, p1_s.at[w, f], p1_r.at[w, f, s, d - 1], ring_dev(s, True, d))

    def second_copy(w, f, s, e, d):
        xx = g if f else og_
        if s == 0:
            blk = W.at[w, xx, ring(y, 4 - e), z, :, cols(s)]
        else:
            blk = W.at[w, xx, y, ring(z, 4 - e), :, cols(s)]
        return rc(blk, blk, p2_s.at[w, f], p2_r.at[w, f, s, d - 1], ring_dev(s, False, d))

    def sib_copy(w, f, s, e):
        blk = plane(w, f, s, e)
        return rc(blk, blk, sb_s.at[w, f], sb_r.at[w, f], sib)

    def gather_first(w, f):
        for d in (1, 3, 2):
            for s in range(2):
                first_copy(w, f, s, d).start()
        for d in (1, 3, 2):
            for s in range(2):
                second_copy(w, f, s, 0, d).start()

    def gather_second(w, f):
        for d in (1, 3, 2):
            for s in range(2):
                first_copy(w, f, s, d).wait_recv()
                for e in (1, 3, 2):
                    second_copy(w, f, s, d, e).start()
        for s in range(2):
            sib_copy(w, f, s, 0).start()

    def gather_third(w, f):
        for d in (1, 3, 2):
            for s in range(2):
                blk = plane(w, f, s, d)
                rc(blk, blk, p2_s.at[w, f], p2_r.at[w, f, s, d - 1], sib).wait_recv()
                sib_copy(w, f, s, d).start()

    def gather_last(w, f):
        blk = W.at[w, g if f else og_, :, :, :, lanes(768 * oc, 768)]
        rc(blk, blk, sb_s.at[w, f], sb_r.at[w, f], sib).wait_recv()

    def gather_sent(w, f):
        blk = W.at[w, 0, 0, 0:3, :, pl.ds(0, 768)]
        rc(blk, blk, p1_s.at[w, f], p1_r.at[w, f, 0, 0], sib).wait_send()
        blk = W.at[w, 0, 0:3, :, :, pl.ds(0, 768)]
        rc(blk, blk, p2_s.at[w, f], p2_r.at[w, f, 0, 0], sib).wait_send()
        blk = W.at[w, 0, :, :, :, pl.ds(0, 768)]
        rc(blk, blk, sb_s.at[w, f], sb_r.at[w, f], sib).wait_send()

    gather_first(0, 0)
    unit_rows(1)
    probs(1, 3)
    gather_second(0, 0)
    probs(3, 6)
    ins[4].wait()
    gather_third(0, 0)
    gather_first(0, 1)
    gather_last(0, 0)

    exs = {}

    def exchange(i, src, dst):
        exs[i] = rc(src, dst, ex_s.at[i], ex_r.at[i], mate)
        exs[i].start()

    def trows(t):
        return pl.ds(256 * t, 256)

    for t in range(2):
        vsend[t] = nt(hid[trows(t), :], W[0, og_].reshape(768, 1536)).astype(BF16)
        exchange(t, vsend.at[t], vrecv.at[t])
    gather_second(0, 1)
    gather_first(1, 0)
    gather_third(0, 1)
    gather_last(0, 1)
    for t in range(2):
        vown[t] = nt(hid[trows(t), :], W[0, g].reshape(768, 1536))
    gather_second(1, 0)
    gather_first(1, 1)
    own_heads = lanes(768 * g, 768)
    mate_heads = lanes(768 * og_, 768)
    for t in range(2):
        exs[t].wait()
        V[trows(t), :] = (vown[t] + vrecv[t].astype(F32)).astype(BF16)

        def fwd(h, carry):
            n = 256 * (t + 1)
            ATT[trows(t), lanes(768 * g + 128 * h, 128)] = nn(
                Pr[h, trows(t), pl.ds(0, n)].astype(BF16), V[pl.ds(0, n), lanes(128 * h, 128)]
            ).astype(BF16)
            return carry

        lax.fori_loop(0, 6, fwd, 0)
        blk = ATT.at[trows(t), own_heads]
        exchange(2 + t, blk, blk)
        if t == 0:
            gather_third(1, 0)
            gather_second(1, 1)
    gather_last(1, 0)
    gather_third(1, 1)
    gather_last(1, 1)

    lane = lax.broadcasted_iota(jnp.int32, (16, 128), 1)

    def row_sums(first, parts):
        acc = jnp.zeros((16, 128), F32)
        for j, v in zip(first, parts):
            acc = jnp.where(lane == j, jnp.sum(v, axis=1, keepdims=True), acc)
        return acc

    def early_sums(i, carry):
        rr = pl.ds(pl.multiple_of(16 * i, 16), 16)
        kh = (1.0 - al[...]) * hid[rr, :].astype(F32)
        mom[rr, :] = row_sums((1, 4), (kh * kh, og[rr, :].astype(F32) * kh))
        return carry

    def late_sums(i, carry):
        rr = pl.ds(pl.multiple_of(16 * i, 16), 16)
        a = al[...]
        p = proj[rr, :]
        ap = a * p
        kh = (1.0 - a) * hid[rr, :].astype(F32)
        parts = (p * p, kh * ap, ap * ap, og[rr, :].astype(F32) * ap)
        mom[rr, :] += row_sums((0, 2, 3, 5), parts)
        return carry

    def apply(i, carry):
        rr = pl.ds(pl.multiple_of(16 * i, 16), 16)
        a = al[...]
        m = mom[rr, :]
        p = proj[rr, :]
        hf = hid[rr, :].astype(F32)
        go = og[rr, :].astype(F32)
        pr, mr, gc, pc = (m[:, j : j + 1] for j in range(4))
        mixed = hf + a * (p * pr - hf)
        og[rr, :] = (mixed * mr).astype(BF16)
        gmix = mr * (go - mixed * gc)
        proj[rr, :] = gmix * (1.0 - a)
        gpb[rr, :] = (pr * (gmix * a - p * pc)).astype(BF16)
        return carry

    def proj_own(t):
        def one(n, carry):
            nc = lanes(384 * n, 384)
            proj[trows(t), nc] = nn(ATT[trows(t), own_heads], W[1, g, :, :, :, nc].reshape(768, 384))
            return carry

        lax.fori_loop(0, 4, one, 0)

    def ga_own(t):
        vown[t] = nt(gpb[trows(t), :], W[1, g].reshape(768, 1536))

    ins[5].wait()
    proj_own(0)
    lax.fori_loop(0, 32, early_sums, 0, unroll=4)
    for t in range(2):
        exs[2 + t].wait()

        def proj_more(n, carry):
            nc = lanes(384 * n, 384)
            proj[trows(t), nc] += nn(ATT[trows(t), mate_heads], W[1, og_, :, :, :, nc].reshape(768, 384))
            return carry

        lax.fori_loop(0, 4, proj_more, 0)
        lax.fori_loop(16 * t, 16 * t + 16, late_sums, 0, unroll=4)
        msend[t] = mom[trows(t), :].T[:8]
        mcp = rc(msend.at[t], mrecv.at[t], nm_s.at[1 + t], nm_r.at[1 + t], mate)
        mcp.start()
        if t == 0:
            proj_own(1)
        mcp.wait()
        m = [msend[t, pl.ds(j, 1), :] + mrecv[t, pl.ds(j, 1), :] for j in range(6)]
        pr = lax.rsqrt(m[0] / D + EPS)
        mr = lax.rsqrt((m[1] + 2.0 * pr * m[2] + pr * pr * m[3]) / D + EPS)
        gm = (m[4] + pr * m[5]) / D
        pm = (mr * m[5] - mr * mr * mr * gm * (m[2] + pr * m[3])) / D
        zero = jnp.zeros_like(pr)
        eight = jnp.concatenate([pr, mr, mr * mr * gm, pr * pr * pm, zero, zero, zero, zero], axis=0)
        mom[trows(t), :] = jnp.concatenate([eight, jnp.zeros((120, 256), F32)], axis=0).T
        lax.fori_loop(16 * t, 16 * t + 16, apply, 0, unroll=4)
        for j in range(2):
            gasend[t, j] = nt(gpb[trows(t), :], W[1, og_, 2 * j : 2 * j + 2].reshape(384, 1536)).astype(BF16)
            exchange(4 + 2 * t + j, gasend.at[t, j], garecv.at[t, j])
        ga_own(t)
    outs = [pltpu.make_async_copy(og, nh_h, out_m.at[0])]
    outs[0].start()

    gsc = {}

    def half(p):
        return g if p == 0 else og_

    def rs_partner(w, p, j, left, right):
        rr = pl.ds(384 * j, 384)
        gss[p, rr, :] = tn(
            left[:, lanes(768 * half(p) + 384 * j, 384)], right[:, lanes(768 * oc, 768)]
        ).astype(BF16)
        gsc[w, p, j] = rc(gss.at[p, rr], gsr.at[w, p, rr], gs_s.at[w, p, j], gs_r.at[w, p, j], sib)
        gsc[w, p, j].start()

    def rs_own(w, p, j, left, right):
        part = tn(left[:, lanes(768 * half(p) + 384 * j, 384)], right[:, lanes(768 * c, 768)])
        gsc[w, p, j].wait()
        total = part + gsr[w, p, pl.ds(384 * j, 384), :].astype(F32)
        RSA[w, p, 2 * j : 2 * j + 2] = total.astype(BF16).reshape(2, 4, 48, 768)

    def rs_first(w, p):
        for d in (1, 3, 2):
            rc(
                RSA.at[w, p, :, ring(z, d), :, pl.ds(0, 384)], r1b.at[w, p, 0, d - 1],
                r1_s.at[w, p], r1_r.at[w, p, 0], zdev(d),
            ).start()
            rc(
                RSA.at[w, p, ring(y, d), :, :, pl.ds(384, 384)], r1b.at[w, p, 1, d - 1],
                r1_s.at[w, p], r1_r.at[w, p, 1], ydev(d),
            ).start()

    def rs_second(w, p):
        for s in range(2):
            rc(r1b.at[w, p, s], r1b.at[w, p, s], r1_s.at[w, p], r1_r.at[w, p, s], sib).wait_recv()
            for b in range(4):
                if s == 0:
                    acc = RSA[w, p, b, z, :, pl.ds(0, 384)].astype(F32)
                else:
                    acc = RSA[w, p, y, b, :, pl.ds(384, 384)].astype(F32)
                for d in range(3):
                    acc += r1b[w, p, s, d, b].astype(F32)
                S1[w, p, s, b] = acc.astype(BF16)
            for d in (1, 3, 2):
                at = ring(y, d) if s == 0 else ring(z, d)
                rc(
                    S1.at[w, p, s, at], r2b.at[w, p, s, d - 1],
                    r2_s.at[w, p], r2_r.at[w, p, s], ring_dev(s, True, d),
                ).start()

    def rs_third(w, p):
        for s in range(2):
            rc(r2b.at[w, p, s], r2b.at[w, p, s], r2_s.at[w, p], r2_r.at[w, p, s], sib).wait_recv()
            acc = S1[w, p, s, y if s == 0 else z].astype(F32)
            for d in range(3):
                acc += r2b[w, p, s, d].astype(F32)
            xk[w, p, :, pl.ds(384 * s, 384)] = acc

    def rs_sent(w, p):
        rc(r1b.at[w, p], r1b.at[w, p], r1_s.at[w, p], r1_r.at[w, p, 0], sib).wait_send()
        rc(r2b.at[w, p], r2b.at[w, p], r2_s.at[w, p], r2_r.at[w, p, 0], sib).wait_send()

    away = jnp.where(x == g, 1, 0)
    mine = pl.ds(pl.multiple_of(24 * c, 8), 24)
    theirs = pl.ds(pl.multiple_of(24 * oc, 8), 24)

    def owner_first(w):
        far = xk[w, away]
        for i in range(2):
            xs[w, i] = far[24 * i : 24 * i + 24].astype(BF16)
        rc(xs.at[w, c], xr.at[w, 0], fd_s.at[w, 0], fd_r.at[w, 0], row(4)).start()
        rc(xs.at[w, oc], xr.at[w, 1], fd_s.at[w, 0], fd_r.at[w, 0], row(6)).start()
        near = xk.at[w, 1 - away]
        rc(near.at[theirs], gpt.at[w], fd_s.at[w, 1], fd_r.at[w, 1], sib).start()
        for i, part in enumerate((near[...], far)):
            dots = jnp.sum(part * U48[w, i], axis=1, keepdims=True)
            rds[w, i] = jnp.broadcast_to(dots, (48, 128))
        for i in range(1, 8):
            rc(
                rds.at[w, 1 if i & 4 else 0, theirs if i & 2 else mine], rdr.at[w, i - 1],
                fd_s.at[w, 2], fd_r.at[w, 2], row(i),
            ).start()

    def owner_last(w, dst, sem):
        rc(rdr.at[w], rdr.at[w], fd_s.at[w, 2], fd_r.at[w, 2], sib).wait()
        dot = rds[w, 0, mine, :]
        for i in range(7):
            dot += rdr[w, i]
        rc(gpt.at[w], gpt.at[w], fd_s.at[w, 1], fd_r.at[w, 1], sib).wait()
        rc(xr.at[w], xr.at[w], fd_s.at[w, 0], fd_r.at[w, 0], sib).wait()
        halves = (xk[w, 1 - away, mine, :] + xr[w, 0].astype(F32), gpt[w] + xr[w, 1].astype(F32))
        for at, part in zip((c, oc), halves):
            nc = lanes(768 * at, 768)
            gown[w, :, nc] = (part - unit[w, :, nc] * dot[:, :1]) / nrm[:, w : w + 1]
        cp = pltpu.make_async_copy(gown.at[w], dst, sem)
        cp.start()
        outs.append(cp)

    def bwd(h, carry):
        hc = lanes(128 * h, 128)
        for r in range(4):
            n = 128 * (r + 1)
            rr = pl.ds(128 * r, 128)
            gp = nt(GA[rr, hc], V[pl.ds(0, n), hc])
            pb = Pr[h, rr, pl.ds(0, n)]
            delta = jnp.sum(pb * gp, axis=1, keepdims=True)
            gs = (pb * (gp - delta)).astype(BF16)
            gsb[rr, pl.ds(0, n)] = gs
            gq[rr, hc] = (nn(gs, k[pl.ds(0, n), hc]) * SCALE).astype(BF16)
        gk[:, hc] = (tn(gsb[...], q[:, hc]) * SCALE).astype(BF16)
        return carry

    def value_grad(h, carry):
        hc = lanes(128 * h, 128)
        GV[:, lanes(768 * g + 128 * h, 128)] = tn(Pr[h].astype(BF16), GA[:, hc]).astype(BF16)
        return carry

    for p in range(2):
        for j in range(2):
            rs_partner(1, p, j, ATT, gpb)
    for p in range(2):
        for j in range(2):
            rs_own(1, p, j, ATT, gpb)
        rs_first(1, p)
    for j in range(2):
        exs[4 + j].wait()
        exs[6 + j].wait()
        jc = pl.ds(384 * j, 384)
        for t in range(2):
            GA[trows(t), jc] = (vown[t, :, jc] + garecv[t, j].astype(F32)).astype(BF16)
        lax.fori_loop(3 * j, 3 * j + 3, value_grad, 0)
        blk = GV.at[:, lanes(768 * g + 384 * j, 384)]
        exchange(8 + j, blk, blk)

    for j in range(2):
        rs_partner(0, 0, j, GV, hid)
    for j in range(2):
        rs_own(0, 0, j, GV, hid)
    rs_first(0, 0)
    lax.fori_loop(0, 1, bwd, 0)
    rs_second(1, 0)
    rs_second(1, 1)
    for j in range(2):
        exs[8 + j].wait()
        rs_partner(0, 1, j, GV, hid)
        rs_own(0, 1, j, GV, hid)
    rs_first(0, 1)

    def hidden_grad(n, carry):
        nc = lanes(384 * n, 384)
        gpb[:, nc] = (proj[:, nc] + nn(GV[...], W[0, :, :, :, :, nc].reshape(1536, 384))).astype(BF16)
        return carry

    rs_second(0, 0)
    rs_third(1, 0)
    rs_third(1, 1)
    owner_first(1)
    lax.fori_loop(1, 4, bwd, 0)
    rs_second(0, 1)
    owner_last(1, gwo_h, out_m.at[4])
    rs_third(0, 0)
    lax.fori_loop(4, 6, bwd, 0)
    outs.append(pltpu.make_async_copy(gq, gq_h, out_m.at[1]))
    outs.append(pltpu.make_async_copy(gk, gk_h, out_m.at[2]))
    outs[-2].start()
    outs[-1].start()
    rs_third(0, 1)
    owner_first(0)
    lax.fori_loop(0, 4, hidden_grad, 0)
    outs.append(pltpu.make_async_copy(gpb, gh_h, out_m.at[3]))
    outs[-1].start()
    owner_last(0, gwv_h, out_m.at[5])
    for w in range(2):
        for f in range(2):
            gather_sent(w, f)
            rs_sent(w, f)
    for cp in outs:
        cp.wait()


def place(*refs):
    src, dst, buf = refs[:6], refs[6:12], refs[12:18]
    sem = refs[18]
    loads = [pltpu.make_async_copy(src[i], buf[i], sem.at[0, i]) for i in range(6)]
    stores = [pltpu.make_async_copy(buf[i], dst[i], sem.at[1, i]) for i in range(6)]
    for cp in loads:
        cp.start()
    for i in range(6):
        loads[i].wait()
        stores[i].start()
    for cp in stores:
        cp.wait()


def shards(hidden, queries, attn_keys, w_value, w_out, alpha, out_grad):
    vm = pltpu.VMEM
    dma = pltpu.SemaphoreType.DMA
    hbm = pl.BlockSpec(memory_space=pltpu.HBM)
    scratch = [
        vm((512, 1536), BF16), vm((512, 768), BF16), vm((512, 768), BF16), vm((512, 1536), BF16),
        vm((2, 24, 1536), BF16), vm((2, 24, 1536), F32), vm((24, 128), F32),
        vm((24, 128), F32), vm((7, 24, 128), F32), vm((2, 3, 24, 768), BF16), vm((2, 2, 48, 768), F32),
        vm((2, 2, 4, 4, 48, 1536), BF16),
        vm((2, 256, 768), BF16), vm((2, 256, 768), BF16), vm((2, 256, 768), F32), vm((512, 768), BF16),
        vm((6, 512, 512), F32), vm((512, 1536), BF16), vm((512, 1536), F32), vm((512, 1536), BF16),
        vm((512, 128), F32), vm((2, 8, 256), F32), vm((2, 8, 256), F32),
        vm((2, 2, 256, 384), BF16), vm((2, 2, 256, 384), BF16), vm((512, 768), BF16), vm((512, 512), BF16),
        vm((512, 768), BF16), vm((512, 768), BF16), vm((512, 1536), BF16),
        vm((2, 768, 768), BF16), vm((2, 2, 768, 768), BF16), vm((2, 2, 4, 4, 48, 768), BF16),
        vm((2, 2, 2, 3, 4, 48, 384), BF16), vm((2, 2, 2, 4, 48, 384), BF16), vm((2, 2, 2, 3, 48, 384), BF16),
        vm((2, 2, 48, 768), F32), vm((2, 2, 24, 768), BF16), vm((2, 2, 24, 768), BF16),
        vm((2, 24, 768), F32), vm((2, 24, 1536), F32), vm((2, 2, 48, 128), F32), vm((2, 7, 24, 128), F32),
        dma((6,)), dma((6,)), dma((3,)), dma((3,)), dma((2,)), dma((2,)),
        dma((2, 2)), dma((2, 2, 2, 3)), dma((2, 2)), dma((2, 2, 2, 3)), dma((2, 2)), dma((2, 2)),
        dma((10,)), dma((10,)), dma((2, 2, 2)), dma((2, 2, 2)),
        dma((2, 2)), dma((2, 2, 2)), dma((2, 2)), dma((2, 2, 2)),
        dma((2, 3)), dma((2, 3)),
    ]
    sds = jax.ShapeDtypeStruct
    shapes = (
        sds((512, 1536), BF16), sds((512, 1536), BF16), sds((512, 768), BF16),
        sds((512, 768), BF16), sds((24, 1536), F32), sds((24, 1536), F32),
    )
    made = pl.pallas_call(
        kernel,
        out_shape=shapes,
        in_specs=[hbm] * 5 + [pl.BlockSpec(memory_space=pltpu.VMEM), hbm],
        out_specs=[hbm] * 6,
        scratch_shapes=scratch,
        compiler_params=pltpu.CompilerParams(
            collective_id=0, has_side_effects=True, vmem_limit_bytes=67043328
        ),
        name="sublayer",
    )(hidden, queries, attn_keys, w_value, w_out, alpha.reshape(1, 1536), out_grad)
    return pl.pallas_call(
        place,
        out_shape=shapes,
        in_specs=[hbm] * 6,
        out_specs=[hbm] * 6,
        scratch_shapes=[vm(v.shape, v.dtype) for v in shapes] + [dma((2, 6))],
        name="place",
    )(*made)


def solution(mesh):
    torus = Mesh(mesh.devices.reshape(2, 4, 4, 2, mesh.shape["grp"]), AXES)
    both = P(FSDP, "grp")
    return jax.shard_map(
        shards,
        mesh=torus,
        in_specs=(both, both, both, both, both, P("grp"), both),
        out_specs=(both,) * 6,
        check_vma=False,
    )
```

```python
import jax
import jax.numpy as jnp
from jax import lax
from jax.experimental import pallas as pl
from jax.experimental.pallas import tpu as pltpu
from jax.sharding import Mesh
from jax.sharding import PartitionSpec as P

D = 3072
EPS = 1e-06
AXES = ("fsdp_0", "fsdp_1", "fsdp_2", "fsdp_3", "grp")
FSDP = AXES[:4]
SCALE = 128 ** (-0.5)
F32 = jnp.float32
BF16 = jnp.bfloat16
MESH = pl.DeviceIdType.MESH


def nt(a, b):
    return lax.dot_general(a, b, (((1,), (1,)), ((), ())), preferred_element_type=F32)


def tn(a, b):
    return lax.dot_general(a, b, (((0,), (0,)), ((), ())), preferred_element_type=F32)


def nn(a, b):
    return lax.dot_general(a, b, (((1,), (0,)), ((), ())), preferred_element_type=F32)


def lanes(start, size):
    return pl.ds(pl.multiple_of(start, 128), size)


def kernel(
    hid_h, q_h, k_h, wv_h, wo_h, al_1, og_h,
    nh_h, gh_h, gq_h, gk_h, gwv_h, gwo_h,
    al, hid, q, k, og, wraw, unit, nrm, nsend, nrecv, rawr, U48, W,
    vsend, vrecv, vown, V, Pr, ATT, proj, gpb, mom, msend, mrecv,
    gasend, garecv, GA, gsb, gq, gk, GV, gss, gsr, RSA, r1b, S1, r2b, xk, xs, xr, gpt, gown, rds, rdr,
    in_m, out_m, nm_s, nm_r, us_s, us_r, p1_s, p1_r, p2_s, p2_r, sb_s, sb_r,
    ex_s, ex_r, gs_s, gs_r, r1_s, r1_r, r2_s, r2_r, fd_s, fd_r,
):
    x, y, z, c, g = (lax.axis_index(a) for a in AXES)
    oc = 1 - c
    og_ = 1 - g

    def ring(v, d):
        return lax.rem(v + d, 4)

    def row(i):
        return (1 - x if i & 4 else x, y, z, oc if i & 2 else c, og_ if i & 1 else g)

    mate = row(1)
    sib = row(2)

    def ydev(d):
        return (x, ring(y, d), z, c, g)

    def zdev(d):
        return (x, y, ring(z, d), c, g)

    def rc(src, dst, ss, rs, dev):
        return pltpu.make_async_remote_copy(
            src_ref=src, dst_ref=dst, send_sem=ss, recv_sem=rs, device_id=dev, device_id_type=MESH
        )

    ins = [
        pltpu.make_async_copy(wv_h, wraw.at[0], in_m.at[0]),
        pltpu.make_async_copy(wo_h, wraw.at[1], in_m.at[1]),
        pltpu.make_async_copy(q_h, q, in_m.at[2]),
        pltpu.make_async_copy(k_h, k, in_m.at[3]),
        pltpu.make_async_copy(hid_h, hid, in_m.at[4]),
        pltpu.make_async_copy(og_h, og, in_m.at[5]),
    ]
    for cp in ins:
        cp.start()

    barrier = pltpu.get_barrier_semaphore()
    peers = [row(i) for i in range(1, 8)] + [ydev(d) for d in (1, 2, 3)] + [zdev(d) for d in (1, 2, 3)]
    for dev in peers:
        pl.semaphore_signal(barrier, inc=1, device_id=dev, device_id_type=MESH)

    gsb[...] = jnp.zeros_like(gsb)
    al[...] = al_1[...].reshape(1, 1536)
    ins[0].wait()
    ins[1].wait()
    lane24 = lax.broadcasted_iota(jnp.int32, (24, 128), 1)
    sq = [jnp.sum(wraw[w].astype(F32) * wraw[w].astype(F32), axis=1, keepdims=True) for w in range(2)]
    nsend[...] = jnp.where(lane24 == 0, sq[0], sq[1])
    pl.semaphore_wait(barrier, len(peers))
    for i in range(1, 8):
        rc(nsend, nrecv.at[i - 1], nm_s.at[0], nm_r.at[0], row(i)).start()
    for w in range(2):
        for j, i in enumerate((2, 4, 6)):
            rc(
                wraw.at[w, :, lanes(768 * (oc if i & 2 else c), 768)], rawr.at[w, j],
                us_s.at[w], us_r.at[w], row(i),
            ).start()

    def probs(first, last):
        def one(h, carry):
            hc = lanes(128 * h, 128)
            for r in range(4):
                n = 128 * (r + 1)
                rr = pl.ds(128 * r, 128)
                s = nt(q[rr, hc], k[pl.ds(0, n), hc]) * SCALE
                row_at = lax.broadcasted_iota(jnp.int32, (128, n), 0) + 128 * r
                col_at = lax.broadcasted_iota(jnp.int32, (128, n), 1)
                s = jnp.where(row_at >= col_at, s, -1e30)
                e = jnp.exp(s - jnp.max(s, axis=1, keepdims=True))
                Pr[h, rr, pl.ds(0, n)] = e / jnp.sum(e, axis=1, keepdims=True)
                if r < 3:
                    Pr[h, rr, pl.ds(n, 512 - n)] = jnp.zeros((128, 512 - n), F32)
            return carry

        lax.fori_loop(first, last, one, 0)

    ins[2].wait()
    ins[3].wait()
    probs(0, 1)

    rc(nrecv, nrecv, nm_s.at[0], nm_r.at[0], sib).wait()
    sq = [nsend[...]] + [nrecv[i] for i in range(7)]
    norms = [jnp.sqrt(sq[2 * i] + sq[2 * i + 1] + EPS) for i in range(4)]
    nrm[...] = norms[0]

    def unit_rows(w):
        rc(rawr.at[w], rawr.at[w], us_s.at[w], us_r.at[w], sib).wait()
        div = [norms[i][:, w : w + 1] for i in range(4)]
        unit[w] = wraw[w].astype(F32) / div[0]
        near = (unit[w, :, lanes(768 * c, 768)], rawr[w, 0].astype(F32) / div[1])
        far = (rawr[w, 1].astype(F32) / div[2], rawr[w, 2].astype(F32) / div[3])
        for i, (mine, other) in enumerate((near, far)):
            low = jnp.where(c == 0, mine, other)
            high = jnp.where(c == 0, other, mine)
            block = jnp.concatenate([low, high], axis=0)
            U48[w, i] = block
            W[w, 1 - x if i else x, y, z, :, lanes(768 * c, 768)] = block.astype(BF16)

    unit_rows(0)

    def cols(s):
        return lanes(768 * c + 384 * s, 384)

    def own_block(w, f, s):
        return W.at[w, g if f else og_, y, z, :, cols(s)]

    def plane(w, f, s, e):
        if s == 0:
            return W.at[w, g if f else og_, :, ring(z, 4 - e), :, cols(s)]
        return W.at[w, g if f else og_, ring(y, 4 - e), :, :, cols(s)]

    def ring_dev(s, first, d):
        return ydev(d) if (s == 0) == first else zdev(d)

    def first_copy(w, f, s, d):
        blk = own_block(w, f, s)
        return rc(blk, blk, p1_s.at[w, f], p1_r.at[w, f, s, d - 1], ring_dev(s, True, d))

    def second_copy(w, f, s, e, d):
        xx = g if f else og_
        if s == 0:
            blk = W.at[w, xx, ring(y, 4 - e), z, :, cols(s)]
        else:
            blk = W.at[w, xx, y, ring(z, 4 - e), :, cols(s)]
        return rc(blk, blk, p2_s.at[w, f], p2_r.at[w, f, s, d - 1], ring_dev(s, False, d))

    def sib_copy(w, f, s, e):
        blk = plane(w, f, s, e)
        return rc(blk, blk, sb_s.at[w, f], sb_r.at[w, f], sib)

    def gather_first(w, f):
        for d in (1, 3, 2):
            for s in range(2):
                first_copy(w, f, s, d).start()

    def gather_own(w, f):
        for d in (1, 3, 2):
            for s in range(2):
                second_copy(w, f, s, 0, d).start()

    def gather_second(w, f):
        for d in (1, 3, 2):
            for s in range(2):
                first_copy(w, f, s, d).wait_recv()
                for e in (1, 3, 2):
                    second_copy(w, f, s, d, e).start()
        for s in range(2):
            sib_copy(w, f, s, 0).start()

    def gather_third(w, f):
        for d in (1, 3, 2):
            for s in range(2):
                blk = plane(w, f, s, d)
                rc(blk, blk, p2_s.at[w, f], p2_r.at[w, f, s, d - 1], sib).wait_recv()
                sib_copy(w, f, s, d).start()

    def gather_last(w, f):
        blk = W.at[w, g if f else og_, :, :, :, lanes(768 * oc, 768)]
        rc(blk, blk, sb_s.at[w, f], sb_r.at[w, f], sib).wait_recv()

    def gather_sent(w, f):
        blk = W.at[w, 0, 0, 0:3, :, pl.ds(0, 768)]
        rc(blk, blk, p1_s.at[w, f], p1_r.at[w, f, 0, 0], sib).wait_send()
        blk = W.at[w, 0, 0:3, :, :, pl.ds(0, 768)]
        rc(blk, blk, p2_s.at[w, f], p2_r.at[w, f, 0, 0], sib).wait_send()
        blk = W.at[w, 0, :, :, :, pl.ds(0, 768)]
        rc(blk, blk, sb_s.at[w, f], sb_r.at[w, f], sib).wait_send()

    gather_first(0, 0)
    gather_own(0, 0)
    unit_rows(1)
    probs(1, 3)
    gather_second(0, 0)
    probs(3, 6)
    gather_first(0, 1)
    ins[4].wait()
    gather_third(0, 0)
    gather_own(0, 1)
    gather_last(0, 0)

    exs = {}

    def exchange(i, src, dst):
        exs[i] = rc(src, dst, ex_s.at[i], ex_r.at[i], mate)
        exs[i].start()

    def trows(t):
        return pl.ds(256 * t, 256)

    for t in range(2):
        vsend[t] = nt(hid[trows(t), :], W[0, og_].reshape(768, 1536)).astype(BF16)
        exchange(t, vsend.at[t], vrecv.at[t])
    gather_second(0, 1)
    gather_first(1, 0)
    gather_own(1, 0)
    gather_first(1, 1)
    gather_third(0, 1)
    gather_second(1, 0)
    gather_own(1, 1)
    gather_second(1, 1)
    gather_last(0, 1)
    for t in range(2):
        vown[t] = nt(hid[trows(t), :], W[0, g].reshape(768, 1536))
    own_heads = lanes(768 * g, 768)
    mate_heads = lanes(768 * og_, 768)
    lane = lax.broadcasted_iota(jnp.int32, (16, 128), 1)

    def row_sums(first, parts):
        acc = jnp.zeros((16, 128), F32)
        for j, v in zip(first, parts):
            acc = jnp.where(lane == j, jnp.sum(v, axis=1, keepdims=True), acc)
        return acc

    def early_sums(i, carry):
        rr = pl.ds(pl.multiple_of(16 * i, 16), 16)
        kh = (1.0 - al[...]) * hid[rr, :].astype(F32)
        mom[rr, :] = row_sums((1, 4), (kh * kh, og[rr, :].astype(F32) * kh))
        return carry

    for t in range(2):
        exs[t].wait()
        V[trows(t), :] = (vown[t] + vrecv[t].astype(F32)).astype(BF16)

        def fwd(h, carry):
            n = 256 * (t + 1)
            ATT[trows(t), lanes(768 * g + 128 * h, 128)] = nn(
                Pr[h, trows(t), pl.ds(0, n)].astype(BF16), V[pl.ds(0, n), lanes(128 * h, 128)]
            ).astype(BF16)
            return carry

        if t == 0:
            lax.fori_loop(0, 6, fwd, 0)
            blk = ATT.at[trows(0), own_heads]
            exchange(2, blk, blk)
            ins[5].wait()
            lax.fori_loop(0, 32, early_sums, 0, unroll=4)
        else:
            lax.fori_loop(0, 3, fwd, 0)
            blk = ATT.at[trows(1), lanes(768 * g, 384)]
            exchange(3, blk, blk)
            lax.fori_loop(3, 6, fwd, 0)
    gather_third(1, 0)
    gather_third(1, 1)
    gather_last(1, 0)
    gather_last(1, 1)

    def late_sums(i, carry):
        rr = pl.ds(pl.multiple_of(16 * i, 16), 16)
        a = al[...]
        p = proj[rr, :]
        ap = a * p
        kh = (1.0 - a) * hid[rr, :].astype(F32)
        parts = (p * p, kh * ap, ap * ap, og[rr, :].astype(F32) * ap)
        mom[rr, :] += row_sums((0, 2, 3, 5), parts)
        return carry

    def apply(i, carry):
        rr = pl.ds(pl.multiple_of(16 * i, 16), 16)
        a = al[...]
        m = mom[rr, :]
        p = proj[rr, :]
        hf = hid[rr, :].astype(F32)
        go = og[rr, :].astype(F32)
        pr, mr, gc, pc = (m[:, j : j + 1] for j in range(4))
        mixed = hf + a * (p * pr - hf)
        og[rr, :] = (mixed * mr).astype(BF16)
        gmix = mr * (go - mixed * gc)
        proj[rr, :] = gmix * (1.0 - a)
        gpb[rr, :] = (pr * (gmix * a - p * pc)).astype(BF16)
        return carry

    def proj_own(t):
        def one(n, carry):
            nc = lanes(384 * n, 384)
            proj[trows(t), nc] = nn(ATT[trows(t), own_heads], W[1, g, :, :, :, nc].reshape(768, 384))
            return carry

        lax.fori_loop(0, 4, one, 0)

    def ga_own(t):
        vown[t] = nt(gpb[trows(t), :], W[1, g].reshape(768, 1536))

    def proj_more(t):
        def one(n, carry):
            nc = lanes(384 * n, 384)
            proj[trows(t), nc] += nn(ATT[trows(t), mate_heads], W[1, og_, :, :, :, nc].reshape(768, 384))
            return carry

        lax.fori_loop(0, 4, one, 0)

    def statistics(t):
        lax.fori_loop(16 * t, 16 * t + 16, late_sums, 0, unroll=4)
        msend[t] = mom[trows(t), :].T[:8]
        cp = rc(msend.at[t], mrecv.at[t], nm_s.at[1 + t], nm_r.at[1 + t], mate)
        cp.start()
        return cp

    def gradients(t, cp):
        cp.wait()
        m = [msend[t, pl.ds(j, 1), :] + mrecv[t, pl.ds(j, 1), :] for j in range(6)]
        pr = lax.rsqrt(m[0] / D + EPS)
        mr = lax.rsqrt((m[1] + 2.0 * pr * m[2] + pr * pr * m[3]) / D + EPS)
        gm = (m[4] + pr * m[5]) / D
        pm = (mr * m[5] - mr * mr * mr * gm * (m[2] + pr * m[3])) / D
        zero = jnp.zeros_like(pr)
        eight = jnp.concatenate([pr, mr, mr * mr * gm, pr * pr * pm, zero, zero, zero, zero], axis=0)
        mom[trows(t), :] = jnp.concatenate([eight, jnp.zeros((120, 256), F32)], axis=0).T
        lax.fori_loop(16 * t, 16 * t + 16, apply, 0, unroll=4)

    def ga_part(t, j):
        gasend[t, j] = nt(gpb[trows(t), :], W[1, og_, 2 * j : 2 * j + 2].reshape(384, 1536)).astype(BF16)

    def ga_exchange(t, j):
        exchange(5 + 2 * t + j, gasend.at[t, j], garecv.at[t, j])

    proj_own(0)
    exs[2].wait_recv()
    proj_more(0)
    stat0 = statistics(0)
    blk = ATT.at[trows(1), lanes(768 * g + 384, 384)]
    exchange(4, blk, blk)
    proj_own(1)
    gradients(0, stat0)
    ga_part(0, 0)
    ga_exchange(0, 0)
    ga_part(0, 1)
    exs[3].wait_recv()
    exs[4].wait_recv()
    proj_more(1)
    stat1 = statistics(1)
    ga_exchange(0, 1)
    ga_own(0)
    gradients(1, stat1)
    for j in range(2):
        ga_part(1, j)
        ga_exchange(1, j)
    ga_own(1)
    for i in range(2, 5):
        exs[i].wait_send()
    outs = [pltpu.make_async_copy(og, nh_h, out_m.at[0])]
    outs[0].start()

    gsc = {}

    def half(p):
        return g if p == 0 else og_

    def rs_partner(w, p, j, left, right):
        rr = pl.ds(384 * j, 384)
        gss[p, rr, :] = tn(
            left[:, lanes(768 * half(p) + 384 * j, 384)], right[:, lanes(768 * oc, 768)]
        ).astype(BF16)
        gsc[w, p, j] = rc(gss.at[p, rr], gsr.at[w, p, rr], gs_s.at[w, p, j], gs_r.at[w, p, j], sib)
        gsc[w, p, j].start()

    def rs_own(w, p, j, left, right):
        part = tn(left[:, lanes(768 * half(p) + 384 * j, 384)], right[:, lanes(768 * c, 768)])
        gsc[w, p, j].wait()
        total = part + gsr[w, p, pl.ds(384 * j, 384), :].astype(F32)
        RSA[w, p, 2 * j : 2 * j + 2] = total.astype(BF16).reshape(2, 4, 48, 768)

    def rs_first(w, p):
        for d in (2, 1, 3):
            rc(
                RSA.at[w, p, :, ring(z, d), :, pl.ds(0, 384)], r1b.at[w, p, 0, d - 1],
                r1_s.at[w, p], r1_r.at[w, p, 0], zdev(d),
            ).start()
            rc(
                RSA.at[w, p, ring(y, d), :, :, pl.ds(384, 384)], r1b.at[w, p, 1, d - 1],
                r1_s.at[w, p], r1_r.at[w, p, 1], ydev(d),
            ).start()

    def rs_second(w, p):
        for s in range(2):
            rc(r1b.at[w, p, s], r1b.at[w, p, s], r1_s.at[w, p], r1_r.at[w, p, s], sib).wait_recv()
            for b in range(4):
                if s == 0:
                    acc = RSA[w, p, b, z, :, pl.ds(0, 384)].astype(F32)
                else:
                    acc = RSA[w, p, y, b, :, pl.ds(384, 384)].astype(F32)
                for d in range(3):
                    acc += r1b[w, p, s, d, b].astype(F32)
                S1[w, p, s, b] = acc.astype(BF16)
            for d in (2, 1, 3):
                at = ring(y, d) if s == 0 else ring(z, d)
                rc(
                    S1.at[w, p, s, at], r2b.at[w, p, s, d - 1],
                    r2_s.at[w, p], r2_r.at[w, p, s], ring_dev(s, True, d),
                ).start()

    def rs_third(w, p):
        for s in range(2):
            rc(r2b.at[w, p, s], r2b.at[w, p, s], r2_s.at[w, p], r2_r.at[w, p, s], sib).wait_recv()
            acc = S1[w, p, s, y if s == 0 else z].astype(F32)
            for d in range(3):
                acc += r2b[w, p, s, d].astype(F32)
            xk[w, p, :, pl.ds(384 * s, 384)] = acc

    def rs_sent(w, p):
        rc(r1b.at[w, p], r1b.at[w, p], r1_s.at[w, p], r1_r.at[w, p, 0], sib).wait_send()
        rc(r2b.at[w, p], r2b.at[w, p], r2_s.at[w, p], r2_r.at[w, p, 0], sib).wait_send()

    away = jnp.where(x == g, 1, 0)
    mine = pl.ds(pl.multiple_of(24 * c, 8), 24)
    theirs = pl.ds(pl.multiple_of(24 * oc, 8), 24)

    def owner_first(w):
        far = xk[w, away]
        near = xk[w, 1 - away]
        for i, part in enumerate((near, far)):
            dots = jnp.sum(part * U48[w, i], axis=1, keepdims=True)
            rds[w, i] = jnp.broadcast_to(dots, (48, 128))
            xs[w, i] = far[24 * i : 24 * i + 24].astype(BF16)

        def send_dots(i):
            rc(
                rds.at[w, 1 if i & 4 else 0, theirs if i & 2 else mine], rdr.at[w, i - 1],
                fd_s.at[w, 2], fd_r.at[w, 2], row(i),
            ).start()

        for i in (1, 3, 5, 7):
            send_dots(i)
        rc(xs.at[w, c], xr.at[w, 0], fd_s.at[w, 0], fd_r.at[w, 0], row(4)).start()
        rc(xs.at[w, oc], xr.at[w, 1], fd_s.at[w, 0], fd_r.at[w, 0], row(6)).start()
        rc(xk.at[w, 1 - away, theirs], gpt.at[w], fd_s.at[w, 1], fd_r.at[w, 1], sib).start()
        for i in (2, 4, 6):
            send_dots(i)

    def owner_last(w, dst, sem):
        rc(rdr.at[w], rdr.at[w], fd_s.at[w, 2], fd_r.at[w, 2], sib).wait()
        dot = rds[w, 0, mine, :]
        for i in range(7):
            dot += rdr[w, i]
        rc(gpt.at[w], gpt.at[w], fd_s.at[w, 1], fd_r.at[w, 1], sib).wait()
        rc(xr.at[w], xr.at[w], fd_s.at[w, 0], fd_r.at[w, 0], sib).wait()
        halves = (xk[w, 1 - away, mine, :] + xr[w, 0].astype(F32), gpt[w] + xr[w, 1].astype(F32))
        for at, part in zip((c, oc), halves):
            nc = lanes(768 * at, 768)
            gown[w, :, nc] = (part - unit[w, :, nc] * dot[:, :1]) / nrm[:, w : w + 1]
        cp = pltpu.make_async_copy(gown.at[w], dst, sem)
        cp.start()
        outs.append(cp)

    def bwd(h, carry):
        hc = lanes(128 * h, 128)
        for r in range(4):
            n = 128 * (r + 1)
            rr = pl.ds(128 * r, 128)
            gp = nt(GA[rr, hc], V[pl.ds(0, n), hc])
            pb = Pr[h, rr, pl.ds(0, n)]
            delta = jnp.sum(pb * gp, axis=1, keepdims=True)
            gs = (pb * (gp - delta)).astype(BF16)
            gsb[rr, pl.ds(0, n)] = gs
            gq[rr, hc] = (nn(gs, k[pl.ds(0, n), hc]) * SCALE).astype(BF16)
        gk[:, hc] = (tn(gsb[...], q[:, hc]) * SCALE).astype(BF16)
        return carry

    def value_grad(h, carry):
        hc = lanes(128 * h, 128)
        GV[:, lanes(768 * g + 128 * h, 128)] = tn(Pr[h].astype(BF16), GA[:, hc]).astype(BF16)
        return carry

    for p in range(2):
        for j in range(2):
            rs_partner(1, p, j, ATT, gpb)
    for p in range(2):
        for j in range(2):
            rs_own(1, p, j, ATT, gpb)
        rs_first(1, p)
    for j in range(2):
        exs[5 + j].wait()
        exs[7 + j].wait()
        jc = pl.ds(384 * j, 384)
        for t in range(2):
            GA[trows(t), jc] = (vown[t, :, jc] + garecv[t, j].astype(F32)).astype(BF16)
        lax.fori_loop(3 * j, 3 * j + 3, value_grad, 0)
        blk = GV.at[:, lanes(768 * g + 384 * j, 384)]
        exchange(9 + j, blk, blk)

    for j in range(2):
        rs_partner(0, 0, j, GV, hid)
    for j in range(2):
        rs_own(0, 0, j, GV, hid)
    rs_first(0, 0)
    lax.fori_loop(0, 2, bwd, 0)
    rs_second(1, 0)
    exs[9].wait()
    rs_partner(0, 1, 0, GV, hid)
    rs_own(0, 1, 0, GV, hid)
    lax.fori_loop(2, 4, bwd, 0)
    rs_second(1, 1)
    rs_second(0, 0)
    exs[10].wait()
    rs_partner(0, 1, 1, GV, hid)
    rs_own(0, 1, 1, GV, hid)
    rs_first(0, 1)

    def hidden_grad(n, carry):
        nc = lanes(384 * n, 384)
        gpb[:, nc] = (proj[:, nc] + nn(GV[...], W[0, :, :, :, :, nc].reshape(1536, 384))).astype(BF16)
        return carry

    rs_third(1, 0)
    rs_third(1, 1)
    owner_first(1)
    rs_third(0, 0)
    lax.fori_loop(0, 4, hidden_grad, 0)
    outs.append(pltpu.make_async_copy(gpb, gh_h, out_m.at[3]))
    outs[-1].start()
    lax.fori_loop(4, 6, bwd, 0)
    outs.append(pltpu.make_async_copy(gq, gq_h, out_m.at[1]))
    outs.append(pltpu.make_async_copy(gk, gk_h, out_m.at[2]))
    outs[-2].start()
    outs[-1].start()
    rs_second(0, 1)
    owner_last(1, gwo_h, out_m.at[4])
    rs_third(0, 1)
    owner_first(0)
    owner_last(0, gwv_h, out_m.at[5])
    for w in range(2):
        for f in range(2):
            gather_sent(w, f)
            rs_sent(w, f)
    for cp in outs:
        cp.wait()


def place(*refs):
    src, dst, buf = refs[:6], refs[6:12], refs[12:18]
    sem = refs[18]
    loads = [pltpu.make_async_copy(src[i], buf[i], sem.at[0, i]) for i in range(6)]
    stores = [pltpu.make_async_copy(buf[i], dst[i], sem.at[1, i]) for i in range(6)]
    for cp in loads:
        cp.start()
    for i in range(6):
        loads[i].wait()
        stores[i].start()
    for cp in stores:
        cp.wait()


def shards(hidden, queries, attn_keys, w_value, w_out, alpha, out_grad):
    vm = pltpu.VMEM
    dma = pltpu.SemaphoreType.DMA
    hbm = pl.BlockSpec(memory_space=pltpu.HBM)
    scratch = [
        vm((1, 1536), F32), vm((512, 1536), BF16), vm((512, 768), BF16), vm((512, 768), BF16), vm((512, 1536), BF16),
        vm((2, 24, 1536), BF16), vm((2, 24, 1536), F32), vm((24, 128), F32),
        vm((24, 128), F32), vm((7, 24, 128), F32), vm((2, 3, 24, 768), BF16), vm((2, 2, 48, 768), F32),
        vm((2, 2, 4, 4, 48, 1536), BF16),
        vm((2, 256, 768), BF16), vm((2, 256, 768), BF16), vm((2, 256, 768), F32), vm((512, 768), BF16),
        vm((6, 512, 512), F32), vm((512, 1536), BF16), vm((512, 1536), F32), vm((512, 1536), BF16),
        vm((512, 128), F32), vm((2, 8, 256), F32), vm((2, 8, 256), F32),
        vm((2, 2, 256, 384), BF16), vm((2, 2, 256, 384), BF16), vm((512, 768), BF16), vm((512, 512), BF16),
        vm((512, 768), BF16), vm((512, 768), BF16), vm((512, 1536), BF16),
        vm((2, 768, 768), BF16), vm((2, 2, 768, 768), BF16), vm((2, 2, 4, 4, 48, 768), BF16),
        vm((2, 2, 2, 3, 4, 48, 384), BF16), vm((2, 2, 2, 4, 48, 384), BF16), vm((2, 2, 2, 3, 48, 384), BF16),
        vm((2, 2, 48, 768), F32), vm((2, 2, 24, 768), BF16), vm((2, 2, 24, 768), BF16),
        vm((2, 24, 768), F32), vm((2, 24, 1536), F32), vm((2, 2, 48, 128), F32), vm((2, 7, 24, 128), F32),
        dma((6,)), dma((6,)), dma((3,)), dma((3,)), dma((2,)), dma((2,)),
        dma((2, 2)), dma((2, 2, 2, 3)), dma((2, 2)), dma((2, 2, 2, 3)), dma((2, 2)), dma((2, 2)),
        dma((11,)), dma((11,)), dma((2, 2, 2)), dma((2, 2, 2)),
        dma((2, 2)), dma((2, 2, 2)), dma((2, 2)), dma((2, 2, 2)),
        dma((2, 3)), dma((2, 3)),
    ]
    sds = jax.ShapeDtypeStruct
    shapes = (
        sds((512, 1536), BF16), sds((512, 1536), BF16), sds((512, 768), BF16),
        sds((512, 768), BF16), sds((24, 1536), F32), sds((24, 1536), F32),
    )
    made = pl.pallas_call(
        kernel,
        out_shape=shapes,
        in_specs=[hbm] * 5 + [pl.BlockSpec(memory_space=pltpu.VMEM), hbm],
        out_specs=[hbm] * 6,
        scratch_shapes=scratch,
        compiler_params=pltpu.CompilerParams(
            collective_id=0, has_side_effects=True, vmem_limit_bytes=67043328
        ),
        name="sublayer",
    )(hidden, queries, attn_keys, w_value, w_out, alpha, out_grad)
    return pl.pallas_call(
        place,
        out_shape=shapes,
        in_specs=[hbm] * 6,
        out_specs=[hbm] * 6,
        scratch_shapes=[vm(v.shape, v.dtype) for v in shapes] + [dma((2, 6))],
        name="place",
    )(*made)


def solution(mesh):
    torus = Mesh(mesh.devices.reshape(2, 4, 4, 2, mesh.shape["grp"]), AXES)
    both = P(FSDP, "grp")
    return jax.shard_map(
        shards,
        mesh=torus,
        in_specs=(both, both, both, both, both, P("grp"), both),
        out_specs=(both,) * 6,
        check_vma=False,
    )
```

```python
import jax
import jax.numpy as jnp
from jax import lax
from jax.experimental import pallas as pl
from jax.experimental.pallas import tpu as pltpu
from jax.sharding import Mesh
from jax.sharding import PartitionSpec as P

D = 3072
EPS = 1e-06
AXES = ("fsdp_0", "fsdp_1", "fsdp_2", "fsdp_3", "grp")
FSDP = AXES[:4]
SCALE = 128 ** (-0.5)
F32 = jnp.float32
BF16 = jnp.bfloat16
MESH = pl.DeviceIdType.MESH


def nt(a, b):
    return lax.dot_general(a, b, (((1,), (1,)), ((), ())), preferred_element_type=F32)


def tn(a, b):
    return lax.dot_general(a, b, (((0,), (0,)), ((), ())), preferred_element_type=F32)


def nn(a, b):
    return lax.dot_general(a, b, (((1,), (0,)), ((), ())), preferred_element_type=F32)


def lanes(start, size):
    return pl.ds(pl.multiple_of(start, 128), size)


def kernel(
    hid_h, q_h, k_h, wv_h, wo_h, al_1, og_h,
    nh_h, gh_h, gq_h, gk_h, gwv_h, gwo_h,
    al, hid, q, k, og, wraw, unit, nrm, nsend, nrecv, rawr, U48, W,
    vsend, vrecv, vown, V, Pr, ATT, proj, gpb, mom, msend, mrecv,
    gasend, garecv, GA, gsb, gq, gk, GV, gss, gsr, RSA, r1b, S1, r2b, xk, xs, xr, gpt, gown, rds, rdr,
    in_m, out_m, nm_s, nm_r, us_s, us_r, p1_s, p1_r, p2_s, p2_r, sb_s, sb_r,
    ex_s, ex_r, gs_s, gs_r, r1_s, r1_r, r2_s, r2_r, fd_s, fd_r,
):
    x, y, z, c, g = (lax.axis_index(a) for a in AXES)
    oc = 1 - c
    og_ = 1 - g

    def ring(v, d):
        return lax.rem(v + d, 4)

    def row(i):
        return (1 - x if i & 4 else x, y, z, oc if i & 2 else c, og_ if i & 1 else g)

    mate = row(1)
    sib = row(2)

    def ydev(d):
        return (x, ring(y, d), z, c, g)

    def zdev(d):
        return (x, y, ring(z, d), c, g)

    def rc(src, dst, ss, rs, dev):
        return pltpu.make_async_remote_copy(
            src_ref=src, dst_ref=dst, send_sem=ss, recv_sem=rs, device_id=dev, device_id_type=MESH
        )

    ins = [
        pltpu.make_async_copy(wv_h, wraw.at[0], in_m.at[0]),
        pltpu.make_async_copy(wo_h, wraw.at[1], in_m.at[1]),
        pltpu.make_async_copy(q_h, q, in_m.at[2]),
        pltpu.make_async_copy(k_h, k, in_m.at[3]),
        pltpu.make_async_copy(hid_h, hid, in_m.at[4]),
        pltpu.make_async_copy(og_h, og, in_m.at[5]),
    ]
    for cp in ins:
        cp.start()

    barrier = pltpu.get_barrier_semaphore()
    peers = [row(i) for i in range(1, 8)] + [ydev(d) for d in (1, 2, 3)] + [zdev(d) for d in (1, 2, 3)]
    for dev in peers:
        pl.semaphore_signal(barrier, inc=1, device_id=dev, device_id_type=MESH)

    gsb[...] = jnp.zeros_like(gsb)
    al[...] = al_1[...].reshape(1, 1536)
    ins[0].wait()
    ins[1].wait()
    lane24 = lax.broadcasted_iota(jnp.int32, (24, 128), 1)
    sq = [jnp.sum(wraw[w].astype(F32) * wraw[w].astype(F32), axis=1, keepdims=True) for w in range(2)]
    nsend[...] = jnp.where(lane24 == 0, sq[0], sq[1])
    pl.semaphore_wait(barrier, len(peers))
    for i in range(1, 8):
        rc(nsend, nrecv.at[i - 1], nm_s.at[0], nm_r.at[0], row(i)).start()
    for w in range(2):
        for j, i in enumerate((2, 4, 6)):
            rc(
                wraw.at[w, :, lanes(768 * (oc if i & 2 else c), 768)], rawr.at[w, j],
                us_s.at[w], us_r.at[w], row(i),
            ).start()

    def probs(first, last):
        def one(h, carry):
            hc = lanes(128 * h, 128)
            for r in range(4):
                n = 128 * (r + 1)
                rr = pl.ds(128 * r, 128)
                s = nt(q[rr, hc], k[pl.ds(0, n), hc]) * SCALE
                row_at = lax.broadcasted_iota(jnp.int32, (128, n), 0) + 128 * r
                col_at = lax.broadcasted_iota(jnp.int32, (128, n), 1)
                s = jnp.where(row_at >= col_at, s, -1e30)
                e = jnp.exp(s - jnp.max(s, axis=1, keepdims=True))
                Pr[h, rr, pl.ds(0, n)] = e / jnp.sum(e, axis=1, keepdims=True)
                if r < 3:
                    Pr[h, rr, pl.ds(n, 512 - n)] = jnp.zeros((128, 512 - n), F32)
            return carry

        lax.fori_loop(first, last, one, 0)

    ins[2].wait()
    ins[3].wait()
    probs(0, 1)

    rc(nrecv, nrecv, nm_s.at[0], nm_r.at[0], sib).wait()
    sq = [nsend[...]] + [nrecv[i] for i in range(7)]
    norms = [jnp.sqrt(sq[2 * i] + sq[2 * i + 1] + EPS) for i in range(4)]
    nrm[...] = norms[0]

    def unit_rows(w):
        rc(rawr.at[w], rawr.at[w], us_s.at[w], us_r.at[w], sib).wait()
        div = [norms[i][:, w : w + 1] for i in range(4)]
        unit[w] = wraw[w].astype(F32) / div[0]
        near = (unit[w, :, lanes(768 * c, 768)], rawr[w, 0].astype(F32) / div[1])
        far = (rawr[w, 1].astype(F32) / div[2], rawr[w, 2].astype(F32) / div[3])
        for i, (mine, other) in enumerate((near, far)):
            low = jnp.where(c == 0, mine, other)
            high = jnp.where(c == 0, other, mine)
            block = jnp.concatenate([low, high], axis=0)
            U48[w, i] = block
            W[w, 1 - x if i else x, y, z, :, lanes(768 * c, 768)] = block.astype(BF16)

    unit_rows(0)

    def cols(s):
        return lanes(768 * c + 384 * s, 384)

    def own_block(w, f, s):
        return W.at[w, g if f else og_, y, z, :, cols(s)]

    def plane(w, f, s, e):
        if s == 0:
            return W.at[w, g if f else og_, :, ring(z, 4 - e), :, cols(s)]
        return W.at[w, g if f else og_, ring(y, 4 - e), :, :, cols(s)]

    def ring_dev(s, first, d):
        return ydev(d) if (s == 0) == first else zdev(d)

    def first_copy(w, f, s, d):
        blk = own_block(w, f, s)
        return rc(blk, blk, p1_s.at[w, f], p1_r.at[w, f, s, d - 1], ring_dev(s, True, d))

    def second_copy(w, f, s, e, d):
        xx = g if f else og_
        if s == 0:
            blk = W.at[w, xx, ring(y, 4 - e), z, :, cols(s)]
        else:
            blk = W.at[w, xx, y, ring(z, 4 - e), :, cols(s)]
        return rc(blk, blk, p2_s.at[w, f], p2_r.at[w, f, s, d - 1], ring_dev(s, False, d))

    def sib_copy(w, f, s, e):
        blk = plane(w, f, s, e)
        return rc(blk, blk, sb_s.at[w, f], sb_r.at[w, f], sib)

    def gather_first(w, f):
        for d in (1, 3, 2):
            for s in range(2):
                first_copy(w, f, s, d).start()

    def gather_own(w, f):
        for d in (1, 3, 2):
            for s in range(2):
                second_copy(w, f, s, 0, d).start()

    def gather_second(w, f):
        for d in (1, 3, 2):
            for s in range(2):
                first_copy(w, f, s, d).wait_recv()
                for e in (1, 3, 2):
                    second_copy(w, f, s, d, e).start()
        for s in range(2):
            sib_copy(w, f, s, 0).start()

    def gather_third(w, f):
        for d in (1, 3, 2):
            for s in range(2):
                blk = plane(w, f, s, d)
                rc(blk, blk, p2_s.at[w, f], p2_r.at[w, f, s, d - 1], sib).wait_recv()
                sib_copy(w, f, s, d).start()

    def gather_last(w, f):
        blk = W.at[w, g if f else og_, :, :, :, lanes(768 * oc, 768)]
        rc(blk, blk, sb_s.at[w, f], sb_r.at[w, f], sib).wait_recv()

    def gather_sent(w, f):
        blk = W.at[w, 0, 0, 0:3, :, pl.ds(0, 768)]
        rc(blk, blk, p1_s.at[w, f], p1_r.at[w, f, 0, 0], sib).wait_send()
        blk = W.at[w, 0, 0:3, :, :, pl.ds(0, 768)]
        rc(blk, blk, p2_s.at[w, f], p2_r.at[w, f, 0, 0], sib).wait_send()
        blk = W.at[w, 0, :, :, :, pl.ds(0, 768)]
        rc(blk, blk, sb_s.at[w, f], sb_r.at[w, f], sib).wait_send()

    gather_first(0, 0)
    gather_own(0, 0)
    unit_rows(1)
    probs(1, 3)
    gather_second(0, 0)
    probs(3, 6)
    gather_first(0, 1)
    ins[4].wait()
    gather_third(0, 0)
    gather_own(0, 1)
    exs = {}

    def exchange(i, src, dst):
        exs[i] = rc(src, dst, ex_s.at[i], ex_r.at[i], mate)
        exs[i].start()

    def trows(t):
        return pl.ds(128 * t, 128)

    def value_part(rows, f, at):
        nc = lanes(768 * at, 768)
        return nt(hid[rows, nc], W[0, g if f else og_, :, :, :, nc].reshape(768, 768))

    for t in range(2):
        rr = pl.ds(256 * t, 256)
        vown[rr, :] = value_part(rr, 0, c)
    gather_second(0, 1)
    gather_first(1, 1)
    gather_first(1, 0)
    gather_last(0, 0)
    for t in range(4):
        vsend[t] = (vown[trows(t), :] + value_part(trows(t), 0, oc)).astype(BF16)
        exchange(t, vsend.at[t], vrecv.at[t])
    gather_third(0, 1)
    gather_own(1, 1)
    gather_second(1, 1)
    gather_own(1, 0)
    gather_second(1, 0)
    gather_last(0, 1)
    for t in range(2):
        rr = pl.ds(256 * t, 256)
        vown[rr, :] = nt(hid[rr, :], W[0, g].reshape(768, 1536))
    own_heads = lanes(768 * g, 768)
    mate_heads = lanes(768 * og_, 768)
    lane = lax.broadcasted_iota(jnp.int32, (16, 128), 1)

    def row_sums(first, parts):
        acc = jnp.zeros((16, 128), F32)
        for j, v in zip(first, parts):
            acc = jnp.where(lane == j, jnp.sum(v, axis=1, keepdims=True), acc)
        return acc

    def early_sums(i, carry):
        rr = pl.ds(pl.multiple_of(16 * i, 16), 16)
        kh = (1.0 - al[...]) * hid[rr, :].astype(F32)
        mom[rr, :] = row_sums((1, 4), (kh * kh, og[rr, :].astype(F32) * kh))
        return carry

    def fwd(t):
        n = 128 * (t + 1)

        def one(h, carry):
            ATT[trows(t), lanes(768 * g + 128 * h, 128)] = nn(
                Pr[h, trows(t), pl.ds(0, n)].astype(BF16), V[pl.ds(0, n), lanes(128 * h, 128)]
            ).astype(BF16)
            return carry

        lax.fori_loop(0, 6, one, 0)

    def attn_exchange(t):
        blk = ATT.at[trows(t), own_heads]
        exchange(4 + t, blk, blk)

    for t in range(4):
        exs[t].wait()
        V[trows(t), :] = (vown[trows(t), :] + vrecv[t].astype(F32)).astype(BF16)
        fwd(t)
        if t < 2:
            attn_exchange(t)
        if t == 0:
            ins[5].wait()
            lax.fori_loop(0, 32, early_sums, 0, unroll=4)
        if t == 2:
            gather_third(1, 1)
    gather_last(1, 1)

    def late_sums(i, carry):
        rr = pl.ds(pl.multiple_of(16 * i, 16), 16)
        a = al[...]
        p = proj[rr, :]
        ap = a * p
        kh = (1.0 - a) * hid[rr, :].astype(F32)
        parts = (p * p, kh * ap, ap * ap, og[rr, :].astype(F32) * ap)
        mom[rr, :] += row_sums((0, 2, 3, 5), parts)
        return carry

    def apply(i, carry):
        rr = pl.ds(pl.multiple_of(16 * i, 16), 16)
        a = al[...]
        m = mom[rr, :]
        p = proj[rr, :]
        hf = hid[rr, :].astype(F32)
        go = og[rr, :].astype(F32)
        pr, mr, gc, pc = (m[:, j : j + 1] for j in range(4))
        mixed = hf + a * (p * pr - hf)
        og[rr, :] = (mixed * mr).astype(BF16)
        gmix = mr * (go - mixed * gc)
        proj[rr, :] = gmix * (1.0 - a)
        gpb[rr, :] = (pr * (gmix * a - p * pc)).astype(BF16)
        return carry

    def proj_own(n, carry):
        nc = lanes(384 * n, 384)
        proj[:, nc] = nn(ATT[:, own_heads], W[1, g, :, :, :, nc].reshape(768, 384))
        return carry

    def proj_more(t):
        def one(n, carry):
            nc = lanes(768 * n, 768)
            proj[trows(t), nc] += nn(ATT[trows(t), mate_heads], W[1, og_, :, :, :, nc].reshape(768, 768))
            return carry

        lax.fori_loop(0, 2, one, 0)

    def statistics(t):
        exs[4 + t].wait_recv()
        proj_more(t)
        lax.fori_loop(8 * t, 8 * t + 8, late_sums, 0, unroll=4)
        msend[t] = mom[trows(t), :].T[:8]
        rc(msend.at[t], mrecv.at[t], nm_s.at[1 + t], nm_r.at[1 + t], mate).start()

    def gradients(t):
        rc(msend.at[t], mrecv.at[t], nm_s.at[1 + t], nm_r.at[1 + t], mate).wait()
        m = [msend[t, pl.ds(j, 1), :] + mrecv[t, pl.ds(j, 1), :] for j in range(6)]
        pr = lax.rsqrt(m[0] / D + EPS)
        mr = lax.rsqrt((m[1] + 2.0 * pr * m[2] + pr * pr * m[3]) / D + EPS)
        gm = (m[4] + pr * m[5]) / D
        pm = (mr * m[5] - mr * mr * mr * gm * (m[2] + pr * m[3])) / D
        zero = jnp.zeros_like(pr)
        eight = jnp.concatenate([pr, mr, mr * mr * gm, pr * pr * pm, zero, zero, zero, zero], axis=0)
        mom[trows(t), :] = jnp.concatenate([eight, jnp.zeros((120, 128), F32)], axis=0).T
        lax.fori_loop(8 * t, 8 * t + 8, apply, 0, unroll=4)
        part = nt(gpb[trows(t), :], W[1, og_].reshape(768, 1536)).astype(BF16)
        gasend[t, 0] = part[:, :384]
        gasend[t, 1] = part[:, 384:]

    def ga_exchange(t, j):
        exchange(8 + 2 * t + j, gasend.at[t, j], garecv.at[t, j])

    lax.fori_loop(0, 4, proj_own, 0)
    gather_third(1, 0)
    gather_last(1, 0)
    statistics(0)
    attn_exchange(2)
    statistics(1)
    attn_exchange(3)
    gradients(0)
    statistics(2)
    ga_exchange(0, 0)
    ga_exchange(0, 1)
    gradients(1)
    statistics(3)
    ga_exchange(1, 0)
    gradients(2)
    ga_exchange(2, 0)
    ga_exchange(1, 1)
    rr = pl.ds(0, 256)
    vown[rr, :] = nt(gpb[rr, :], W[1, g].reshape(768, 1536))
    gradients(3)
    ga_exchange(3, 0)
    ga_exchange(2, 1)
    ga_exchange(3, 1)
    rr = pl.ds(256, 256)
    vown[rr, :] = nt(gpb[rr, :], W[1, g].reshape(768, 1536))
    for t in range(4):
        exs[4 + t].wait_send()
    outs = [pltpu.make_async_copy(og, nh_h, out_m.at[0])]
    outs[0].start()

    gsc = {}

    def half(p):
        return g if p == 0 else og_

    def rs_partner(w, p, lo, hi, left, right):
        rr = pl.ds(lo, hi - lo)
        gss[p, rr, :] = tn(
            left[:, lanes(768 * half(p) + lo, hi - lo)], right[:, lanes(768 * oc, 768)]
        ).astype(BF16)
        i = {0: 0, 384: 1, 640: 2}[lo]
        gsc[w, p, lo] = rc(gss.at[p, rr], gsr.at[w, p, rr], gs_s.at[w, p, i], gs_r.at[w, p, i], sib)
        gsc[w, p, lo].start()

    def rs_own(w, p, lo, hi, left, right):
        part = tn(left[:, lanes(768 * half(p) + lo, hi - lo)], right[:, lanes(768 * c, 768)])
        gsc[w, p, lo].wait()
        total = (part + gsr[w, p, pl.ds(lo, hi - lo), :].astype(F32)).astype(BF16)
        at = lo
        while at < hi:
            n = min(48 - at % 48, hi - at)
            b = at // 48
            RSA[w, p, b // 4, b % 4, pl.ds(at % 48, n), :] = total[at - lo : at - lo + n]
            at += n

    def rs_first(w, p):
        for d in (2, 1, 3):
            rc(
                RSA.at[w, p, :, ring(z, d), :, pl.ds(0, 384)], r1b.at[w, p, 0, d - 1],
                r1_s.at[w, p], r1_r.at[w, p, 0], zdev(d),
            ).start()
            rc(
                RSA.at[w, p, ring(y, d), :, :, pl.ds(384, 384)], r1b.at[w, p, 1, d - 1],
                r1_s.at[w, p], r1_r.at[w, p, 1], ydev(d),
            ).start()

    def rs_second(w, p):
        for s in range(2):
            rc(r1b.at[w, p, s], r1b.at[w, p, s], r1_s.at[w, p], r1_r.at[w, p, s], sib).wait_recv()
            for b in range(4):
                if s == 0:
                    acc = RSA[w, p, b, z, :, pl.ds(0, 384)].astype(F32)
                else:
                    acc = RSA[w, p, y, b, :, pl.ds(384, 384)].astype(F32)
                for d in range(3):
                    acc += r1b[w, p, s, d, b].astype(F32)
                S1[w, p, s, b] = acc.astype(BF16)
            for d in (2, 1, 3):
                at = ring(y, d) if s == 0 else ring(z, d)
                rc(
                    S1.at[w, p, s, at], r2b.at[w, p, s, d - 1],
                    r2_s.at[w, p], r2_r.at[w, p, s], ring_dev(s, True, d),
                ).start()

    def rs_third(w, p):
        for s in range(2):
            rc(r2b.at[w, p, s], r2b.at[w, p, s], r2_s.at[w, p], r2_r.at[w, p, s], sib).wait_recv()
            acc = S1[w, p, s, y if s == 0 else z].astype(F32)
            for d in range(3):
                acc += r2b[w, p, s, d].astype(F32)
            xk[w, p, :, pl.ds(384 * s, 384)] = acc

    def rs_sent(w, p):
        rc(r1b.at[w, p], r1b.at[w, p], r1_s.at[w, p], r1_r.at[w, p, 0], sib).wait_send()
        rc(r2b.at[w, p], r2b.at[w, p], r2_s.at[w, p], r2_r.at[w, p, 0], sib).wait_send()

    away = jnp.where(x == g, 1, 0)
    mine = pl.ds(pl.multiple_of(24 * c, 8), 24)
    theirs = pl.ds(pl.multiple_of(24 * oc, 8), 24)

    def owner_first(w):
        far = xk[w, away]
        near = xk[w, 1 - away]
        for i, part in enumerate((near, far)):
            dots = jnp.sum(part * U48[w, i], axis=1, keepdims=True)
            rds[w, i] = jnp.broadcast_to(dots, (48, 128))
            xs[w, i] = far[24 * i : 24 * i + 24].astype(BF16)

        def send_dots(i):
            rc(
                rds.at[w, 1 if i & 4 else 0, theirs if i & 2 else mine], rdr.at[w, i - 1],
                fd_s.at[w, 2], fd_r.at[w, 2], row(i),
            ).start()

        for i in (1, 3, 5, 7):
            send_dots(i)
        rc(xs.at[w, c], xr.at[w, 0], fd_s.at[w, 0], fd_r.at[w, 0], row(4)).start()
        rc(xs.at[w, oc], xr.at[w, 1], fd_s.at[w, 0], fd_r.at[w, 0], row(6)).start()
        rc(xk.at[w, 1 - away, theirs], gpt.at[w], fd_s.at[w, 1], fd_r.at[w, 1], sib).start()
        for i in (2, 4, 6):
            send_dots(i)

    def owner_last(w, dst, sem):
        rc(rdr.at[w], rdr.at[w], fd_s.at[w, 2], fd_r.at[w, 2], sib).wait()
        dot = rds[w, 0, mine, :]
        for i in range(7):
            dot += rdr[w, i]
        rc(gpt.at[w], gpt.at[w], fd_s.at[w, 1], fd_r.at[w, 1], sib).wait()
        rc(xr.at[w], xr.at[w], fd_s.at[w, 0], fd_r.at[w, 0], sib).wait()
        halves = (xk[w, 1 - away, mine, :] + xr[w, 0].astype(F32), gpt[w] + xr[w, 1].astype(F32))
        for at, part in zip((c, oc), halves):
            nc = lanes(768 * at, 768)
            gown[w, :, nc] = (part - unit[w, :, nc] * dot[:, :1]) / nrm[:, w : w + 1]
        cp = pltpu.make_async_copy(gown.at[w], dst, sem)
        cp.start()
        outs.append(cp)

    def bwd(h, carry):
        hc = lanes(128 * h, 128)
        for r in range(4):
            n = 128 * (r + 1)
            rr = pl.ds(128 * r, 128)
            gp = nt(GA[rr, hc], V[pl.ds(0, n), hc])
            pb = Pr[h, rr, pl.ds(0, n)]
            delta = jnp.sum(pb * gp, axis=1, keepdims=True)
            gs = (pb * (gp - delta)).astype(BF16)
            gsb[rr, pl.ds(0, n)] = gs
            gq[rr, hc] = (nn(gs, k[pl.ds(0, n), hc]) * SCALE).astype(BF16)
        gk[:, hc] = (tn(gsb[...], q[:, hc]) * SCALE).astype(BF16)
        return carry

    def value_grad(h, carry):
        hc = lanes(128 * h, 128)
        GV[:, lanes(768 * g + 128 * h, 128)] = tn(Pr[h].astype(BF16), GA[:, hc]).astype(BF16)
        return carry

    for j in range(2):
        for lo in (0, 384):
            rs_partner(1, j, lo, lo + 384, ATT, gpb)
        for lo in (0, 384):
            rs_own(1, j, lo, lo + 384, ATT, gpb)
        rs_first(1, j)
        for t in range(4):
            exs[8 + 2 * t + j].wait()
        jc = pl.ds(384 * j, 384)
        for t in range(4):
            GA[trows(t), jc] = (vown[trows(t), jc] + garecv[t, j].astype(F32)).astype(BF16)
        lax.fori_loop(3 * j, 2 * j + 3, value_grad, 0)
        blk = GV.at[:, lanes(768 * g + 384 * j, 384 - 128 * j)]
        exchange(16 + j, blk, blk)
    value_grad(5, 0)
    blk = GV.at[:, lanes(768 * g + 640, 128)]
    exchange(18, blk, blk)

    for lo in (0, 384):
        rs_partner(0, 0, lo, lo + 384, GV, hid)
    for lo in (0, 384):
        rs_own(0, 0, lo, lo + 384, GV, hid)
    rs_first(0, 0)
    lax.fori_loop(0, 2, bwd, 0)
    rs_second(1, 0)
    exs[16].wait()
    rs_partner(0, 1, 0, 384, GV, hid)
    rs_own(0, 1, 0, 384, GV, hid)
    exs[17].wait()
    rs_partner(0, 1, 384, 640, GV, hid)
    rs_own(0, 1, 384, 640, GV, hid)
    exs[18].wait()
    rs_partner(0, 1, 640, 768, GV, hid)
    rs_own(0, 1, 640, 768, GV, hid)
    rs_first(0, 1)

    def hidden_grad(n, carry):
        nc = lanes(384 * n, 384)
        gpb[:, nc] = (proj[:, nc] + nn(GV[...], W[0, :, :, :, :, nc].reshape(1536, 384))).astype(BF16)
        return carry

    lax.fori_loop(0, 4, hidden_grad, 0)
    outs.append(pltpu.make_async_copy(gpb, gh_h, out_m.at[3]))
    outs[-1].start()
    rs_second(1, 1)
    rs_second(0, 0)
    rs_third(1, 0)
    lax.fori_loop(2, 5, bwd, 0)
    rs_second(0, 1)
    rs_third(1, 1)
    owner_first(1)
    rs_third(0, 0)
    lax.fori_loop(5, 6, bwd, 0)
    outs.append(pltpu.make_async_copy(gq, gq_h, out_m.at[1]))
    outs.append(pltpu.make_async_copy(gk, gk_h, out_m.at[2]))
    outs[-2].start()
    outs[-1].start()
    rs_third(0, 1)
    owner_first(0)
    owner_last(1, gwo_h, out_m.at[4])
    owner_last(0, gwv_h, out_m.at[5])
    for w in range(2):
        for f in range(2):
            gather_sent(w, f)
            rs_sent(w, f)
    for cp in outs:
        cp.wait()


def place(*refs):
    src, dst, buf = refs[:6], refs[6:12], refs[12:18]
    sem = refs[18]
    loads = [pltpu.make_async_copy(src[i], buf[i], sem.at[0, i]) for i in range(6)]
    stores = [pltpu.make_async_copy(buf[i], dst[i], sem.at[1, i]) for i in range(6)]
    for cp in loads:
        cp.start()
    for i in range(6):
        loads[i].wait()
        stores[i].start()
    for cp in stores:
        cp.wait()


def shards(hidden, queries, attn_keys, w_value, w_out, alpha, out_grad):
    vm = pltpu.VMEM
    dma = pltpu.SemaphoreType.DMA
    hbm = pl.BlockSpec(memory_space=pltpu.HBM)
    scratch = [
        vm((1, 1536), F32), vm((512, 1536), BF16), vm((512, 768), BF16), vm((512, 768), BF16), vm((512, 1536), BF16),
        vm((2, 24, 1536), BF16), vm((2, 24, 1536), F32), vm((24, 128), F32),
        vm((24, 128), F32), vm((7, 24, 128), F32), vm((2, 3, 24, 768), BF16), vm((2, 2, 48, 768), F32),
        vm((2, 2, 4, 4, 48, 1536), BF16),
        vm((4, 128, 768), BF16), vm((4, 128, 768), BF16), vm((512, 768), F32), vm((512, 768), BF16),
        vm((6, 512, 512), F32), vm((512, 1536), BF16), vm((512, 1536), F32), vm((512, 1536), BF16),
        vm((512, 128), F32), vm((4, 8, 128), F32), vm((4, 8, 128), F32),
        vm((4, 2, 128, 384), BF16), vm((4, 2, 128, 384), BF16), vm((512, 768), BF16), vm((512, 512), BF16),
        vm((512, 768), BF16), vm((512, 768), BF16), vm((512, 1536), BF16),
        vm((2, 768, 768), BF16), vm((2, 2, 768, 768), BF16), vm((2, 2, 4, 4, 48, 768), BF16),
        vm((2, 2, 2, 3, 4, 48, 384), BF16), vm((2, 2, 2, 4, 48, 384), BF16), vm((2, 2, 2, 3, 48, 384), BF16),
        vm((2, 2, 48, 768), F32), vm((2, 2, 24, 768), BF16), vm((2, 2, 24, 768), BF16),
        vm((2, 24, 768), F32), vm((2, 24, 1536), F32), vm((2, 2, 48, 128), F32), vm((2, 7, 24, 128), F32),
        dma((6,)), dma((6,)), dma((5,)), dma((5,)), dma((2,)), dma((2,)),
        dma((2, 2)), dma((2, 2, 2, 3)), dma((2, 2)), dma((2, 2, 2, 3)), dma((2, 2)), dma((2, 2)),
        dma((19,)), dma((19,)), dma((2, 2, 3)), dma((2, 2, 3)),
        dma((2, 2)), dma((2, 2, 2)), dma((2, 2)), dma((2, 2, 2)),
        dma((2, 3)), dma((2, 3)),
    ]
    sds = jax.ShapeDtypeStruct
    shapes = (
        sds((512, 1536), BF16), sds((512, 1536), BF16), sds((512, 768), BF16),
        sds((512, 768), BF16), sds((24, 1536), F32), sds((24, 1536), F32),
    )
    made = pl.pallas_call(
        kernel,
        out_shape=shapes,
        in_specs=[hbm] * 5 + [pl.BlockSpec(memory_space=pltpu.VMEM), hbm],
        out_specs=[hbm] * 6,
        scratch_shapes=scratch,
        compiler_params=pltpu.CompilerParams(
            collective_id=0, has_side_effects=True, vmem_limit_bytes=67043328
        ),
        name="sublayer",
    )(hidden, queries, attn_keys, w_value, w_out, alpha, out_grad)
    return pl.pallas_call(
        place,
        out_shape=shapes,
        in_specs=[hbm] * 6,
        out_specs=[hbm] * 6,
        scratch_shapes=[vm(v.shape, v.dtype) for v in shapes] + [dma((2, 6))],
        name="place",
    )(*made)


def solution(mesh):
    torus = Mesh(mesh.devices.reshape(2, 4, 4, 2, mesh.shape["grp"]), AXES)
    both = P(FSDP, "grp")
    return jax.shard_map(
        shards,
        mesh=torus,
        in_specs=(both, both, both, both, both, P("grp"), both),
        out_specs=(both,) * 6,
        check_vma=False,
    )
```

```python
import jax
import jax.numpy as jnp
from jax import lax
from jax.experimental import pallas as pl
from jax.experimental.pallas import tpu as pltpu
from jax.sharding import Mesh
from jax.sharding import PartitionSpec as P

D = 3072
EPS = 1e-06
AXES = ("fsdp_0", "fsdp_1", "fsdp_2", "fsdp_3", "grp")
FSDP = AXES[:4]
SCALE = 128 ** (-0.5)
F32 = jnp.float32
BF16 = jnp.bfloat16
MESH = pl.DeviceIdType.MESH


def nt(a, b):
    return lax.dot_general(a, b, (((1,), (1,)), ((), ())), preferred_element_type=F32)


def tn(a, b):
    return lax.dot_general(a, b, (((0,), (0,)), ((), ())), preferred_element_type=F32)


def nn(a, b):
    return lax.dot_general(a, b, (((1,), (0,)), ((), ())), preferred_element_type=F32)


def lanes(start, size):
    return pl.ds(pl.multiple_of(start, 128), size)


def kernel(
    hid_h, q_h, k_h, wv_h, wo_h, al_1, og_h,
    nh_h, gh_h, gq_h, gk_h, gwv_h, gwo_h,
    al, hid, q, k, og, wraw, unit, nrm, nsend, nrecv, rawr, U48, W,
    vsend, vrecv, vown, V, Pr, ATT, proj, gpb, mom, msend, mrecv,
    gasend, garecv, GA, gsb, gq, gk, GV, gss, gsr, RSA, r1b, S1, r2b, xk, xs, xr, gpt, gown, rds, rdr,
    in_m, out_m, nm_s, nm_r, us_s, us_r, p1_s, p1_r, p2_s, p2_r, sb_s, sb_r,
    ex_s, ex_r, gs_s, gs_r, r1_s, r1_r, r2_s, r2_r, fd_s, fd_r,
):
    x, y, z, c, g = (lax.axis_index(a) for a in AXES)
    oc = 1 - c
    og_ = 1 - g

    def ring(v, d):
        return lax.rem(v + d, 4)

    def row(i):
        return (1 - x if i & 4 else x, y, z, oc if i & 2 else c, og_ if i & 1 else g)

    mate = row(1)
    sib = row(2)

    def ydev(d):
        return (x, ring(y, d), z, c, g)

    def zdev(d):
        return (x, y, ring(z, d), c, g)

    def rc(src, dst, ss, rs, dev):
        return pltpu.make_async_remote_copy(
            src_ref=src, dst_ref=dst, send_sem=ss, recv_sem=rs, device_id=dev, device_id_type=MESH
        )

    ins = [
        pltpu.make_async_copy(wv_h, wraw.at[0], in_m.at[0]),
        pltpu.make_async_copy(wo_h, wraw.at[1], in_m.at[1]),
        pltpu.make_async_copy(q_h, q, in_m.at[2]),
        pltpu.make_async_copy(k_h, k, in_m.at[3]),
        pltpu.make_async_copy(hid_h, hid, in_m.at[4]),
        pltpu.make_async_copy(og_h, og, in_m.at[5]),
    ]
    for cp in ins:
        cp.start()

    barrier = pltpu.get_barrier_semaphore()
    peers = [row(i) for i in range(1, 8)] + [ydev(d) for d in (1, 2, 3)] + [zdev(d) for d in (1, 2, 3)]
    for dev in peers:
        pl.semaphore_signal(barrier, inc=1, device_id=dev, device_id_type=MESH)

    gsb[...] = jnp.zeros_like(gsb)
    al[...] = al_1[...].reshape(1, 1536)
    ins[0].wait()
    ins[1].wait()
    lane24 = lax.broadcasted_iota(jnp.int32, (24, 128), 1)
    sq = [jnp.sum(wraw[w].astype(F32) * wraw[w].astype(F32), axis=1, keepdims=True) for w in range(2)]
    sums = jnp.where(lane24 == 0, sq[0], sq[1])
    nsend[...] = jnp.concatenate([sums, jnp.zeros((104, 128), F32)], axis=0).T[:8]
    pl.semaphore_wait(barrier, len(peers))
    for i in range(1, 8):
        rc(nsend, nrecv.at[i - 1], nm_s.at[0], nm_r.at[0], row(i)).start()
    for w in range(2):
        for j, i in enumerate((2, 4, 6)):
            rc(
                wraw.at[w, :, lanes(768 * (oc if i & 2 else c), 768)], rawr.at[w, j],
                us_s.at[w], us_r.at[w], row(i),
            ).start()

    def probs(first, last):
        def one(h, carry):
            hc = lanes(128 * h, 128)
            for r in range(4):
                n = 128 * (r + 1)
                rr = pl.ds(128 * r, 128)
                s = nt(q[rr, hc], k[pl.ds(0, n), hc]) * SCALE
                row_at = lax.broadcasted_iota(jnp.int32, (128, n), 0) + 128 * r
                col_at = lax.broadcasted_iota(jnp.int32, (128, n), 1)
                s = jnp.where(row_at >= col_at, s, -1e30)
                e = jnp.exp(s - jnp.max(s, axis=1, keepdims=True))
                Pr[h, rr, pl.ds(0, n)] = e / jnp.sum(e, axis=1, keepdims=True)
                if r < 3:
                    Pr[h, rr, pl.ds(n, 512 - n)] = jnp.zeros((128, 512 - n), F32)
            return carry

        lax.fori_loop(first, last, one, 0)

    ins[2].wait()
    ins[3].wait()
    probs(0, 1)

    rc(nrecv, nrecv, nm_s.at[0], nm_r.at[0], sib).wait()
    sq = [nsend[...]] + [nrecv[i] for i in range(7)]
    norms = [jnp.sqrt(sq[2 * i] + sq[2 * i + 1] + EPS) for i in range(4)]
    norms = jnp.concatenate(norms + [jnp.zeros((96, 128), F32)], axis=0).T[:24]
    nrm[...] = norms

    def unit_rows(w):
        rc(rawr.at[w], rawr.at[w], us_s.at[w], us_r.at[w], sib).wait()
        div = [norms[:, 8 * i + w : 8 * i + w + 1] for i in range(4)]
        unit[w] = wraw[w].astype(F32) / div[0]
        near = (unit[w, :, lanes(768 * c, 768)], rawr[w, 0].astype(F32) / div[1])
        far = (rawr[w, 1].astype(F32) / div[2], rawr[w, 2].astype(F32) / div[3])
        for i, (mine, other) in enumerate((near, far)):
            low = jnp.where(c == 0, mine, other)
            high = jnp.where(c == 0, other, mine)
            block = jnp.concatenate([low, high], axis=0)
            U48[w, i] = block
            W[w, 1 - x if i else x, y, z, :, lanes(768 * c, 768)] = block.astype(BF16)

    unit_rows(0)

    def cols(s):
        return lanes(768 * c + 384 * s, 384)

    def own_block(w, f, s):
        return W.at[w, g if f else og_, y, z, :, cols(s)]

    def plane(w, f, s, e):
        if s == 0:
            return W.at[w, g if f else og_, :, ring(z, 4 - e), :, cols(s)]
        return W.at[w, g if f else og_, ring(y, 4 - e), :, :, cols(s)]

    def ring_dev(s, first, d):
        return ydev(d) if (s == 0) == first else zdev(d)

    def first_copy(w, f, s, d):
        blk = own_block(w, f, s)
        return rc(blk, blk, p1_s.at[w, f], p1_r.at[w, f, s, d - 1], ring_dev(s, True, d))

    def second_copy(w, f, s, e, d):
        xx = g if f else og_
        if s == 0:
            blk = W.at[w, xx, ring(y, 4 - e), z, :, cols(s)]
        else:
            blk = W.at[w, xx, y, ring(z, 4 - e), :, cols(s)]
        return rc(blk, blk, p2_s.at[w, f], p2_r.at[w, f, s, d - 1], ring_dev(s, False, d))

    def relay_copy(w, f, s, e, d):
        xx = g if f else og_
        if s == 0:
            blk = W.at[w, xx, ring(y, 4 - e), ring(z, 4 - d), :, cols(s)]
        else:
            blk = W.at[w, xx, ring(y, 4 - d), ring(z, 4 - e), :, cols(s)]
        return rc(blk, blk, p2_s.at[w, f], p2_r.at[w, f, s, 1], ring_dev(s, False, d))

    def steps(w):
        return (1, 3) if w else (1, 3, 2)

    def sib_copy(w, f, s, e):
        blk = plane(w, f, s, e)
        return rc(blk, blk, sb_s.at[w, f], sb_r.at[w, f], sib)

    def gather_first(w, f):
        for d in (1, 3, 2):
            for s in range(2):
                first_copy(w, f, s, d).start()

    def gather_own(w, f):
        for d in steps(w):
            for s in range(2):
                second_copy(w, f, s, 0, d).start()

    def gather_second(w, f):
        for d in (1, 3, 2):
            for s in range(2):
                first_copy(w, f, s, d).wait_recv()
                for e in steps(w):
                    second_copy(w, f, s, d, e).start()
        for s in range(2):
            sib_copy(w, f, s, 0).start()

    def gather_third(w, f, dirs=(1, 3, 2)):
        for d in dirs:
            for s in range(2):
                blk = plane(w, f, s, d)
                rc(blk, blk, p2_s.at[w, f], p2_r.at[w, f, s, d - 1], sib).wait_recv()
                if w and d != 2:
                    for e in (0, 1) if d == 1 else (2, 3):
                        relay_copy(w, f, s, e, d).start()
                sib_copy(w, f, s, d).start()

    def gather_last(w, f):
        blk = W.at[w, g if f else og_, :, :, :, lanes(768 * oc, 768)]
        rc(blk, blk, sb_s.at[w, f], sb_r.at[w, f], sib).wait_recv()

    def gather_sent(w, f):
        blk = W.at[w, 0, 0, 0:3, :, pl.ds(0, 768)]
        rc(blk, blk, p1_s.at[w, f], p1_r.at[w, f, 0, 0], sib).wait_send()
        blk = W.at[w, 0, 0:3, :, :, pl.ds(0, 768)]
        rc(blk, blk, p2_s.at[w, f], p2_r.at[w, f, 0, 0], sib).wait_send()
        blk = W.at[w, 0, :, :, :, pl.ds(0, 768)]
        rc(blk, blk, sb_s.at[w, f], sb_r.at[w, f], sib).wait_send()

    gather_first(0, 0)
    gather_own(0, 0)
    unit_rows(1)
    probs(1, 3)
    gather_second(0, 0)
    probs(3, 6)
    gather_first(0, 1)
    ins[4].wait()
    gather_third(0, 0)
    gather_own(0, 1)
    exs = {}

    def exchange(i, src, dst):
        exs[i] = rc(src, dst, ex_s.at[i], ex_r.at[i], mate)
        exs[i].start()

    def trows(t):
        return pl.ds(128 * t, 128)

    def value_part(rows, f, at):
        nc = lanes(768 * at, 768)
        return nt(hid[rows, nc], W[0, g if f else og_, :, :, :, nc].reshape(768, 768))

    for t in range(2):
        rr = pl.ds(256 * t, 256)
        vown[rr, :] = value_part(rr, 0, c)
    gather_second(0, 1)
    gather_first(1, 1)
    gather_first(1, 0)
    gather_last(0, 0)
    for t in range(4):
        vsend[t] = (vown[trows(t), :] + value_part(trows(t), 0, oc)).astype(BF16)
        exchange(t, vsend.at[t], vrecv.at[t])
    gather_third(0, 1)
    gather_own(1, 1)
    gather_second(1, 1)
    gather_own(1, 0)
    gather_second(1, 0)
    gather_last(0, 1)
    for t in range(2):
        rr = pl.ds(256 * t, 256)
        vown[rr, :] = nt(hid[rr, :], W[0, g].reshape(768, 1536))
    own_heads = lanes(768 * g, 768)
    mate_heads = lanes(768 * og_, 768)
    lane = lax.broadcasted_iota(jnp.int32, (16, 128), 1)

    def row_sums(first, parts):
        acc = jnp.zeros((16, 128), F32)
        for j, v in zip(first, parts):
            acc = jnp.where(lane == j, jnp.sum(v, axis=1, keepdims=True), acc)
        return acc

    def early_sums(i, carry):
        rr = pl.ds(pl.multiple_of(16 * i, 16), 16)
        kh = (1.0 - al[...]) * hid[rr, :].astype(F32)
        mom[rr, :] = row_sums((1, 4), (kh * kh, og[rr, :].astype(F32) * kh))
        return carry

    def fwd(t):
        n = 128 * (t + 1)

        def one(h, carry):
            ATT[trows(t), lanes(768 * g + 128 * h, 128)] = nn(
                Pr[h, trows(t), pl.ds(0, n)].astype(BF16), V[pl.ds(0, n), lanes(128 * h, 128)]
            ).astype(BF16)
            return carry

        lax.fori_loop(0, 6, one, 0)

    def attn_exchange(t):
        blk = ATT.at[trows(t), own_heads]
        exchange(4 + t, blk, blk)

    for t in range(4):
        exs[t].wait()
        V[trows(t), :] = (vown[trows(t), :] + vrecv[t].astype(F32)).astype(BF16)
        fwd(t)
        if t < 2:
            attn_exchange(t)
        if t == 0:
            ins[5].wait()
            lax.fori_loop(0, 32, early_sums, 0, unroll=4)
        if t == 1:
            gather_third(1, 1, (1, 3))
        if t == 2:
            gather_third(1, 0, (1, 3))
            gather_third(1, 1, (2,))
    gather_last(1, 1)

    def late_sums(i, carry):
        rr = pl.ds(pl.multiple_of(16 * i, 16), 16)
        a = al[...]
        p = proj[rr, :]
        ap = a * p
        kh = (1.0 - a) * hid[rr, :].astype(F32)
        parts = (p * p, kh * ap, ap * ap, og[rr, :].astype(F32) * ap)
        mom[rr, :] += row_sums((0, 2, 3, 5), parts)
        return carry

    def apply(i, carry):
        rr = pl.ds(pl.multiple_of(16 * i, 16), 16)
        a = al[...]
        m = mom[rr, :]
        p = proj[rr, :]
        hf = hid[rr, :].astype(F32)
        go = og[rr, :].astype(F32)
        pr, mr, gc, pc = (m[:, j : j + 1] for j in range(4))
        mixed = hf + a * (p * pr - hf)
        og[rr, :] = (mixed * mr).astype(BF16)
        gmix = mr * (go - mixed * gc)
        proj[rr, :] = gmix * (1.0 - a)
        gpb[rr, :] = (pr * (gmix * a - p * pc)).astype(BF16)
        return carry

    def proj_own(n, carry):
        nc = lanes(384 * n, 384)
        proj[:, nc] = nn(ATT[:, own_heads], W[1, g, :, :, :, nc].reshape(768, 384))
        return carry

    def proj_more(t):
        def one(n, carry):
            nc = lanes(768 * n, 768)
            proj[trows(t), nc] += nn(ATT[trows(t), mate_heads], W[1, og_, :, :, :, nc].reshape(768, 768))
            return carry

        lax.fori_loop(0, 2, one, 0)

    def statistics(t):
        exs[4 + t].wait_recv()
        proj_more(t)
        lax.fori_loop(8 * t, 8 * t + 8, late_sums, 0, unroll=4)
        msend[t] = mom[trows(t), :].T[:8]
        rc(msend.at[t], mrecv.at[t], nm_s.at[1 + t], nm_r.at[1 + t], mate).start()

    def gradients(t):
        rc(msend.at[t], mrecv.at[t], nm_s.at[1 + t], nm_r.at[1 + t], mate).wait()
        m = [msend[t, pl.ds(j, 1), :] + mrecv[t, pl.ds(j, 1), :] for j in range(6)]
        pr = lax.rsqrt(m[0] / D + EPS)
        mr = lax.rsqrt((m[1] + 2.0 * pr * m[2] + pr * pr * m[3]) / D + EPS)
        gm = (m[4] + pr * m[5]) / D
        pm = (mr * m[5] - mr * mr * mr * gm * (m[2] + pr * m[3])) / D
        zero = jnp.zeros_like(pr)
        eight = jnp.concatenate([pr, mr, mr * mr * gm, pr * pr * pm, zero, zero, zero, zero], axis=0)
        mom[trows(t), :] = jnp.concatenate([eight, jnp.zeros((120, 128), F32)], axis=0).T
        lax.fori_loop(8 * t, 8 * t + 8, apply, 0, unroll=4)
        part = nt(gpb[trows(t), :], W[1, og_].reshape(768, 1536)).astype(BF16)
        gasend[t, 0] = part[:, :384]
        gasend[t, 1] = part[:, 384:]

    def ga_exchange(t, j):
        exchange(8 + 2 * t + j, gasend.at[t, j], garecv.at[t, j])

    lax.fori_loop(0, 4, proj_own, 0)
    gather_third(1, 0, (2,))
    gather_last(1, 0)
    statistics(0)
    attn_exchange(2)
    statistics(1)
    attn_exchange(3)
    gradients(0)
    statistics(2)
    ga_exchange(0, 0)
    ga_exchange(0, 1)
    gradients(1)
    statistics(3)
    ga_exchange(1, 0)
    gradients(2)
    ga_exchange(2, 0)
    ga_exchange(1, 1)
    rr = pl.ds(0, 256)
    vown[rr, :] = nt(gpb[rr, :], W[1, g].reshape(768, 1536))
    gradients(3)
    ga_exchange(3, 0)
    ga_exchange(2, 1)
    ga_exchange(3, 1)
    rr = pl.ds(256, 256)
    vown[rr, :] = nt(gpb[rr, :], W[1, g].reshape(768, 1536))
    for t in range(4):
        exs[4 + t].wait_send()
    outs = [pltpu.make_async_copy(og, nh_h, out_m.at[0])]
    outs[0].start()

    gsc = {}

    def half(p):
        return g if p == 0 else og_

    def rs_partner(w, p, lo, hi, left, right):
        rr = pl.ds(lo, hi - lo)
        gss[p, rr, :] = tn(
            left[:, lanes(768 * half(p) + lo, hi - lo)], right[:, lanes(768 * oc, 768)]
        ).astype(BF16)
        i = {0: 0, 384: 1, 640: 2}[lo]
        gsc[w, p, lo] = rc(gss.at[p, rr], gsr.at[w, p, rr], gs_s.at[w, p, i], gs_r.at[w, p, i], sib)
        gsc[w, p, lo].start()

    def rs_own(w, p, lo, hi, left, right):
        part = tn(left[:, lanes(768 * half(p) + lo, hi - lo)], right[:, lanes(768 * c, 768)])
        gsc[w, p, lo].wait()
        total = (part + gsr[w, p, pl.ds(lo, hi - lo), :].astype(F32)).astype(BF16)
        at = lo
        while at < hi:
            n = min(48 - at % 48, hi - at)
            b = at // 48
            RSA[w, p, b // 4, b % 4, pl.ds(at % 48, n), :] = total[at - lo : at - lo + n]
            at += n

    def rs_first(w, p):
        for d in (2, 1, 3):
            rc(
                RSA.at[w, p, :, ring(z, d), :, pl.ds(0, 384)], r1b.at[w, p, 0, d - 1],
                r1_s.at[w, p], r1_r.at[w, p, 0], zdev(d),
            ).start()
            rc(
                RSA.at[w, p, ring(y, d), :, :, pl.ds(384, 384)], r1b.at[w, p, 1, d - 1],
                r1_s.at[w, p], r1_r.at[w, p, 1], ydev(d),
            ).start()

    def rs_second(w, p):
        for s in range(2):
            rc(r1b.at[w, p, s], r1b.at[w, p, s], r1_s.at[w, p], r1_r.at[w, p, s], sib).wait_recv()
            for b in range(4):
                if s == 0:
                    acc = RSA[w, p, b, z, :, pl.ds(0, 384)].astype(F32)
                else:
                    acc = RSA[w, p, y, b, :, pl.ds(384, 384)].astype(F32)
                for d in range(3):
                    acc += r1b[w, p, s, d, b].astype(F32)
                S1[w, p, s, b] = acc.astype(BF16)
            for d in (2, 1, 3):
                at = ring(y, d) if s == 0 else ring(z, d)
                rc(
                    S1.at[w, p, s, at], r2b.at[w, p, s, d - 1],
                    r2_s.at[w, p], r2_r.at[w, p, s], ring_dev(s, True, d),
                ).start()

    def rs_third(w, p):
        for s in range(2):
            rc(r2b.at[w, p, s], r2b.at[w, p, s], r2_s.at[w, p], r2_r.at[w, p, s], sib).wait_recv()
            acc = S1[w, p, s, y if s == 0 else z].astype(F32)
            for d in range(3):
                acc += r2b[w, p, s, d].astype(F32)
            xk[w, p, :, pl.ds(384 * s, 384)] = acc

    def rs_sent(w, p):
        rc(r1b.at[w, p], r1b.at[w, p], r1_s.at[w, p], r1_r.at[w, p, 0], sib).wait_send()
        rc(r2b.at[w, p], r2b.at[w, p], r2_s.at[w, p], r2_r.at[w, p, 0], sib).wait_send()

    away = jnp.where(x == g, 1, 0)
    mine = pl.ds(pl.multiple_of(24 * c, 8), 24)
    theirs = pl.ds(pl.multiple_of(24 * oc, 8), 24)

    def owner_first(w):
        far = xk[w, away]
        near = xk[w, 1 - away]
        for i, part in enumerate((near, far)):
            dots = jnp.sum(part * U48[w, i], axis=1, keepdims=True)
            rds[w, i] = jnp.broadcast_to(dots, (48, 128))
            xs[w, i] = far[24 * i : 24 * i + 24].astype(BF16)

        def send_dots(i):
            rc(
                rds.at[w, 1 if i & 4 else 0, theirs if i & 2 else mine], rdr.at[w, i - 1],
                fd_s.at[w, 2], fd_r.at[w, 2], row(i),
            ).start()

        for i in (1, 3, 5, 7):
            send_dots(i)
        rc(xs.at[w, c], xr.at[w, 0], fd_s.at[w, 0], fd_r.at[w, 0], row(4)).start()
        rc(xs.at[w, oc], xr.at[w, 1], fd_s.at[w, 0], fd_r.at[w, 0], row(6)).start()
        rc(xk.at[w, 1 - away, theirs], gpt.at[w], fd_s.at[w, 1], fd_r.at[w, 1], sib).start()
        for i in (2, 4, 6):
            send_dots(i)

    def owner_last(w, dst, sem):
        rc(rdr.at[w], rdr.at[w], fd_s.at[w, 2], fd_r.at[w, 2], sib).wait()
        dot = rds[w, 0, mine, :]
        for i in range(7):
            dot += rdr[w, i]
        rc(gpt.at[w], gpt.at[w], fd_s.at[w, 1], fd_r.at[w, 1], sib).wait()
        rc(xr.at[w], xr.at[w], fd_s.at[w, 0], fd_r.at[w, 0], sib).wait()
        halves = (xk[w, 1 - away, mine, :] + xr[w, 0].astype(F32), gpt[w] + xr[w, 1].astype(F32))
        for at, part in zip((c, oc), halves):
            nc = lanes(768 * at, 768)
            gown[w, :, nc] = (part - unit[w, :, nc] * dot[:, :1]) / nrm[:, w : w + 1]
        cp = pltpu.make_async_copy(gown.at[w], dst, sem)
        cp.start()
        outs.append(cp)

    def bwd(h, carry):
        hc = lanes(128 * h, 128)
        for r in range(4):
            n = 128 * (r + 1)
            rr = pl.ds(128 * r, 128)
            gp = nt(GA[rr, hc], V[pl.ds(0, n), hc])
            pb = Pr[h, rr, pl.ds(0, n)]
            delta = jnp.sum(pb * gp, axis=1, keepdims=True)
            gs = (pb * (gp - delta)).astype(BF16)
            gsb[rr, pl.ds(0, n)] = gs
            gq[rr, hc] = (nn(gs, k[pl.ds(0, n), hc]) * SCALE).astype(BF16)
        gk[:, hc] = (tn(gsb[...], q[:, hc]) * SCALE).astype(BF16)
        return carry

    def value_grad(h, carry):
        hc = lanes(128 * h, 128)
        GV[:, lanes(768 * g + 128 * h, 128)] = tn(Pr[h].astype(BF16), GA[:, hc]).astype(BF16)
        return carry

    for j in range(2):
        for lo in (0, 384):
            rs_partner(1, j, lo, lo + 384, ATT, gpb)
        for lo in (0, 384):
            rs_own(1, j, lo, lo + 384, ATT, gpb)
        rs_first(1, j)
        for t in range(4):
            exs[8 + 2 * t + j].wait()
        jc = pl.ds(384 * j, 384)
        for t in range(4):
            GA[trows(t), jc] = (vown[trows(t), jc] + garecv[t, j].astype(F32)).astype(BF16)
        lax.fori_loop(3 * j, 2 * j + 3, value_grad, 0)
        blk = GV.at[:, lanes(768 * g + 384 * j, 384 - 128 * j)]
        exchange(16 + j, blk, blk)
    value_grad(5, 0)
    blk = GV.at[:, lanes(768 * g + 640, 128)]
    exchange(18, blk, blk)

    for lo in (0, 384):
        rs_partner(0, 0, lo, lo + 384, GV, hid)
    for lo in (0, 384):
        rs_own(0, 0, lo, lo + 384, GV, hid)
    rs_first(0, 0)
    lax.fori_loop(0, 2, bwd, 0)
    rs_second(1, 0)
    exs[16].wait()
    rs_partner(0, 1, 0, 384, GV, hid)
    rs_own(0, 1, 0, 384, GV, hid)
    exs[17].wait()
    rs_partner(0, 1, 384, 640, GV, hid)
    rs_own(0, 1, 384, 640, GV, hid)
    exs[18].wait()
    rs_partner(0, 1, 640, 768, GV, hid)
    rs_own(0, 1, 640, 768, GV, hid)
    rs_first(0, 1)

    def hidden_grad(n, carry):
        nc = lanes(384 * n, 384)
        gpb[:, nc] = (proj[:, nc] + nn(GV[...], W[0, :, :, :, :, nc].reshape(1536, 384))).astype(BF16)
        return carry

    lax.fori_loop(0, 4, hidden_grad, 0)
    outs.append(pltpu.make_async_copy(gpb, gh_h, out_m.at[3]))
    outs[-1].start()
    rs_second(1, 1)
    rs_second(0, 0)
    rs_third(1, 0)
    lax.fori_loop(2, 5, bwd, 0)
    rs_second(0, 1)
    rs_third(1, 1)
    owner_first(1)
    rs_third(0, 0)
    lax.fori_loop(5, 6, bwd, 0)
    outs.append(pltpu.make_async_copy(gq, gq_h, out_m.at[1]))
    outs.append(pltpu.make_async_copy(gk, gk_h, out_m.at[2]))
    outs[-2].start()
    outs[-1].start()
    rs_third(0, 1)
    owner_first(0)
    owner_last(1, gwo_h, out_m.at[4])
    owner_last(0, gwv_h, out_m.at[5])
    for w in range(2):
        for f in range(2):
            gather_sent(w, f)
            rs_sent(w, f)
    for cp in outs:
        cp.wait()


def place(*refs):
    src, dst, buf = refs[:6], refs[6:12], refs[12:18]
    sem = refs[18]
    loads = [pltpu.make_async_copy(src[i], buf[i], sem.at[0, i]) for i in range(6)]
    stores = [pltpu.make_async_copy(buf[i], dst[i], sem.at[1, i]) for i in range(6)]
    for cp in loads:
        cp.start()
    for i in range(6):
        loads[i].wait()
        stores[i].start()
    for cp in stores:
        cp.wait()


def shards(hidden, queries, attn_keys, w_value, w_out, alpha, out_grad):
    vm = pltpu.VMEM
    dma = pltpu.SemaphoreType.DMA
    hbm = pl.BlockSpec(memory_space=pltpu.HBM)
    scratch = [
        vm((1, 1536), F32), vm((512, 1536), BF16), vm((512, 768), BF16), vm((512, 768), BF16), vm((512, 1536), BF16),
        vm((2, 24, 1536), BF16), vm((2, 24, 1536), F32), vm((24, 128), F32),
        vm((8, 128), F32), vm((7, 8, 128), F32), vm((2, 3, 24, 768), BF16), vm((2, 2, 48, 768), F32),
        vm((2, 2, 4, 4, 48, 1536), BF16),
        vm((4, 128, 768), BF16), vm((4, 128, 768), BF16), vm((512, 768), F32), vm((512, 768), BF16),
        vm((6, 512, 512), F32), vm((512, 1536), BF16), vm((512, 1536), F32), vm((512, 1536), BF16),
        vm((512, 128), F32), vm((4, 8, 128), F32), vm((4, 8, 128), F32),
        vm((4, 2, 128, 384), BF16), vm((4, 2, 128, 384), BF16), vm((512, 768), BF16), vm((512, 512), BF16),
        vm((512, 768), BF16), vm((512, 768), BF16), vm((512, 1536), BF16),
        vm((2, 768, 768), BF16), vm((2, 2, 768, 768), BF16), vm((2, 2, 4, 4, 48, 768), BF16),
        vm((2, 2, 2, 3, 4, 48, 384), BF16), vm((2, 2, 2, 4, 48, 384), BF16), vm((2, 2, 2, 3, 48, 384), BF16),
        vm((2, 2, 48, 768), F32), vm((2, 2, 24, 768), BF16), vm((2, 2, 24, 768), BF16),
        vm((2, 24, 768), F32), vm((2, 24, 1536), F32), vm((2, 2, 48, 128), F32), vm((2, 7, 24, 128), F32),
        dma((6,)), dma((6,)), dma((5,)), dma((5,)), dma((2,)), dma((2,)),
        dma((2, 2)), dma((2, 2, 2, 3)), dma((2, 2)), dma((2, 2, 2, 3)), dma((2, 2)), dma((2, 2)),
        dma((19,)), dma((19,)), dma((2, 2, 3)), dma((2, 2, 3)),
        dma((2, 2)), dma((2, 2, 2)), dma((2, 2)), dma((2, 2, 2)),
        dma((2, 3)), dma((2, 3)),
    ]
    sds = jax.ShapeDtypeStruct
    shapes = (
        sds((512, 1536), BF16), sds((512, 1536), BF16), sds((512, 768), BF16),
        sds((512, 768), BF16), sds((24, 1536), F32), sds((24, 1536), F32),
    )
    made = pl.pallas_call(
        kernel,
        out_shape=shapes,
        in_specs=[hbm] * 5 + [pl.BlockSpec(memory_space=pltpu.VMEM), hbm],
        out_specs=[hbm] * 6,
        scratch_shapes=scratch,
        compiler_params=pltpu.CompilerParams(
            collective_id=0, has_side_effects=True, vmem_limit_bytes=67043328
        ),
        name="sublayer",
    )(hidden, queries, attn_keys, w_value, w_out, alpha, out_grad)
    return pl.pallas_call(
        place,
        out_shape=shapes,
        in_specs=[hbm] * 6,
        out_specs=[hbm] * 6,
        scratch_shapes=[vm(v.shape, v.dtype) for v in shapes] + [dma((2, 6))],
        name="place",
    )(*made)


def solution(mesh):
    torus = Mesh(mesh.devices.reshape(2, 4, 4, 2, mesh.shape["grp"]), AXES)
    both = P(FSDP, "grp")
    return jax.shard_map(
        shards,
        mesh=torus,
        in_specs=(both, both, both, both, both, P("grp"), both),
        out_specs=(both,) * 6,
        check_vma=False,
    )
```

```python
import jax
import jax.numpy as jnp
from jax import lax
from jax.experimental import pallas as pl
from jax.experimental.pallas import tpu as pltpu
from jax.sharding import Mesh
from jax.sharding import PartitionSpec as P

D = 3072
EPS = 1e-06
AXES = ("fsdp_0", "fsdp_1", "fsdp_2", "fsdp_3", "grp")
FSDP = AXES[:4]
SCALE = 128 ** (-0.5)
F32 = jnp.float32
BF16 = jnp.bfloat16
MESH = pl.DeviceIdType.MESH


def nt(a, b):
    return lax.dot_general(a, b, (((1,), (1,)), ((), ())), preferred_element_type=F32)


def tn(a, b):
    return lax.dot_general(a, b, (((0,), (0,)), ((), ())), preferred_element_type=F32)


def nn(a, b):
    return lax.dot_general(a, b, (((1,), (0,)), ((), ())), preferred_element_type=F32)


def lanes(start, size):
    return pl.ds(pl.multiple_of(start, 128), size)


def kernel(
    hid_h, q_h, k_h, wv_h, wo_h, al_1, og_h,
    nh_h, gh_h, gq_h, gk_h, gwv_h, gwo_h,
    al, hid, q, k, og, wraw, unit, nrm, nsend, nrecv, rawr, U48, W,
    vsend, vrecv, vown, V, Pr, ATT, proj, gpb, mom, msend, mrecv,
    gasend, garecv, GA, gsb, gq, gk, GV, gss, gsr, RSA, r1b, S1, r2b, xk, xs, xr, gpt, gown, rds, rdr,
    in_m, out_m, nm_s, nm_r, us_s, us_r, p1_s, p1_r, p2_s, p2_r, sb_s, sb_r,
    ex_s, ex_r, gs_s, gs_r, r1_s, r1_r, r2_s, r2_r, fd_s, fd_r,
):
    x, y, z, c, g = (lax.axis_index(a) for a in AXES)
    oc = 1 - c
    og_ = 1 - g

    def ring(v, d):
        return lax.rem(v + d, 4)

    def row(i):
        return (1 - x if i & 4 else x, y, z, oc if i & 2 else c, og_ if i & 1 else g)

    mate = row(1)
    sib = row(2)

    def ydev(d):
        return (x, ring(y, d), z, c, g)

    def zdev(d):
        return (x, y, ring(z, d), c, g)

    def rc(src, dst, ss, rs, dev):
        return pltpu.make_async_remote_copy(
            src_ref=src, dst_ref=dst, send_sem=ss, recv_sem=rs, device_id=dev, device_id_type=MESH
        )

    ins = [
        pltpu.make_async_copy(wv_h, wraw.at[0], in_m.at[0]),
        pltpu.make_async_copy(wo_h, wraw.at[1], in_m.at[1]),
        pltpu.make_async_copy(q_h, q, in_m.at[2]),
        pltpu.make_async_copy(k_h, k, in_m.at[3]),
        pltpu.make_async_copy(hid_h, hid, in_m.at[4]),
        pltpu.make_async_copy(og_h, og, in_m.at[5]),
    ]
    for cp in ins:
        cp.start()

    barrier = pltpu.get_barrier_semaphore()
    peers = [row(i) for i in range(1, 8)] + [ydev(d) for d in (1, 2, 3)] + [zdev(d) for d in (1, 2, 3)]
    for dev in peers:
        pl.semaphore_signal(barrier, inc=1, device_id=dev, device_id_type=MESH)

    gsb[...] = jnp.zeros_like(gsb)
    al[...] = al_1[...].reshape(1, 1536)
    ins[0].wait()
    ins[1].wait()
    lane24 = lax.broadcasted_iota(jnp.int32, (24, 128), 1)
    sq = [jnp.sum(wraw[w].astype(F32) * wraw[w].astype(F32), axis=1, keepdims=True) for w in range(2)]
    sums = jnp.where(lane24 == 0, sq[0], sq[1])
    nsend[...] = jnp.concatenate([sums, jnp.zeros((104, 128), F32)], axis=0).T[:8]
    pl.semaphore_wait(barrier, len(peers))
    for i in range(1, 8):
        rc(nsend, nrecv.at[i - 1], nm_s.at[0], nm_r.at[0], row(i)).start()
    for w in range(2):
        for j, i in enumerate((2, 4, 6)):
            rc(
                wraw.at[w, :, lanes(768 * (oc if i & 2 else c), 768)], rawr.at[w, j],
                us_s.at[w], us_r.at[w], row(i),
            ).start()

    def probs(first, last):
        def one(h, carry):
            hc = lanes(128 * h, 128)
            for r in range(4):
                n = 128 * (r + 1)
                rr = pl.ds(128 * r, 128)
                s = nt(q[rr, hc], k[pl.ds(0, n), hc]) * SCALE
                row_at = lax.broadcasted_iota(jnp.int32, (128, n), 0) + 128 * r
                col_at = lax.broadcasted_iota(jnp.int32, (128, n), 1)
                s = jnp.where(row_at >= col_at, s, -1e30)
                e = jnp.exp(s - jnp.max(s, axis=1, keepdims=True))
                Pr[h, rr, pl.ds(0, n)] = e / jnp.sum(e, axis=1, keepdims=True)
                if r < 3:
                    Pr[h, rr, pl.ds(n, 512 - n)] = jnp.zeros((128, 512 - n), F32)
            return carry

        lax.fori_loop(first, last, one, 0)

    ins[2].wait()
    ins[3].wait()
    probs(0, 1)

    rc(nrecv, nrecv, nm_s.at[0], nm_r.at[0], sib).wait()
    sq = [nsend[...]] + [nrecv[i] for i in range(7)]
    norms = [jnp.sqrt(sq[2 * i] + sq[2 * i + 1] + EPS) for i in range(4)]
    norms = jnp.concatenate(norms + [jnp.zeros((96, 128), F32)], axis=0).T[:24]
    nrm[...] = norms

    def unit_rows(w):
        rc(rawr.at[w], rawr.at[w], us_s.at[w], us_r.at[w], sib).wait()
        div = [norms[:, 8 * i + w : 8 * i + w + 1] for i in range(4)]
        unit[w] = wraw[w].astype(F32) / div[0]
        near = (unit[w, :, lanes(768 * c, 768)], rawr[w, 0].astype(F32) / div[1])
        far = (rawr[w, 1].astype(F32) / div[2], rawr[w, 2].astype(F32) / div[3])
        for i, (mine, other) in enumerate((near, far)):
            low = jnp.where(c == 0, mine, other)
            high = jnp.where(c == 0, other, mine)
            block = jnp.concatenate([low, high], axis=0)
            U48[w, i] = block
            W[w, 1 - x if i else x, y, z, :, lanes(768 * c, 768)] = block.astype(BF16)

    unit_rows(0)

    def cols(s):
        return lanes(768 * c + 384 * s, 384)

    def own_block(w, f, s):
        return W.at[w, g if f else og_, y, z, :, cols(s)]

    def plane(w, f, s, e):
        if s == 0:
            return W.at[w, g if f else og_, :, ring(z, 4 - e), :, cols(s)]
        return W.at[w, g if f else og_, ring(y, 4 - e), :, :, cols(s)]

    def ring_dev(s, first, d):
        return ydev(d) if (s == 0) == first else zdev(d)

    def first_copy(w, f, s, d):
        blk = own_block(w, f, s)
        return rc(blk, blk, p1_s.at[w, f], p1_r.at[w, f, s, d - 1], ring_dev(s, True, d))

    def second_copy(w, f, s, e, d):
        xx = g if f else og_
        if s == 0:
            blk = W.at[w, xx, ring(y, 4 - e), z, :, cols(s)]
        else:
            blk = W.at[w, xx, y, ring(z, 4 - e), :, cols(s)]
        return rc(blk, blk, p2_s.at[w, f], p2_r.at[w, f, s, d - 1], ring_dev(s, False, d))

    def relay_copy(w, f, s, e, d):
        xx = g if f else og_
        if s == 0:
            blk = W.at[w, xx, ring(y, 4 - e), ring(z, 4 - d), :, cols(s)]
        else:
            blk = W.at[w, xx, ring(y, 4 - d), ring(z, 4 - e), :, cols(s)]
        return rc(blk, blk, p2_s.at[w, f], p2_r.at[w, f, s, 1], ring_dev(s, False, d))

    def steps(w):
        return (1, 3) if w else (1, 3, 2)

    def sib_copy(w, f, s, e):
        blk = plane(w, f, s, e)
        return rc(blk, blk, sb_s.at[w, f], sb_r.at[w, f], sib)

    def gather_first(w, f):
        for d in (1, 3, 2):
            for s in range(2):
                first_copy(w, f, s, d).start()

    def gather_own(w, f):
        for d in steps(w):
            for s in range(2):
                second_copy(w, f, s, 0, d).start()

    def gather_second(w, f):
        for d in (1, 3, 2):
            for s in range(2):
                first_copy(w, f, s, d).wait_recv()
                for e in steps(w):
                    second_copy(w, f, s, d, e).start()
        for s in range(2):
            sib_copy(w, f, s, 0).start()

    def gather_third(w, f, dirs=(1, 3, 2)):
        for d in dirs:
            for s in range(2):
                blk = plane(w, f, s, d)
                rc(blk, blk, p2_s.at[w, f], p2_r.at[w, f, s, d - 1], sib).wait_recv()
                if w and d != 2:
                    for e in (0, 1) if d == 1 else (2, 3):
                        relay_copy(w, f, s, e, d).start()
                sib_copy(w, f, s, d).start()

    def gather_last(w, f):
        blk = W.at[w, g if f else og_, :, :, :, lanes(768 * oc, 768)]
        rc(blk, blk, sb_s.at[w, f], sb_r.at[w, f], sib).wait_recv()

    def gather_sent(w, f):
        blk = W.at[w, 0, 0, 0:3, :, pl.ds(0, 768)]
        rc(blk, blk, p1_s.at[w, f], p1_r.at[w, f, 0, 0], sib).wait_send()
        blk = W.at[w, 0, 0:3, :, :, pl.ds(0, 768)]
        rc(blk, blk, p2_s.at[w, f], p2_r.at[w, f, 0, 0], sib).wait_send()
        blk = W.at[w, 0, :, :, :, pl.ds(0, 768)]
        rc(blk, blk, sb_s.at[w, f], sb_r.at[w, f], sib).wait_send()

    gather_first(0, 0)
    gather_own(0, 0)
    unit_rows(1)
    probs(1, 3)
    gather_second(0, 0)
    probs(3, 6)
    gather_first(0, 1)
    ins[4].wait()
    gather_third(0, 0)
    gather_own(0, 1)
    exs = {}

    def exchange(i, src, dst):
        exs[i] = rc(src, dst, ex_s.at[i], ex_r.at[i], mate)
        exs[i].start()

    def trows(t):
        return pl.ds(128 * t, 128)

    def value_part(rows, f, at):
        nc = lanes(768 * at, 768)
        return nt(hid[rows, nc], W[0, g if f else og_, :, :, :, nc].reshape(768, 768))

    for t in range(2):
        rr = pl.ds(256 * t, 256)
        vown[rr, :] = value_part(rr, 0, c)
    gather_second(0, 1)
    gather_first(1, 1)
    gather_first(1, 0)
    gather_last(0, 0)
    for t in range(4):
        vsend[t] = (vown[trows(t), :] + value_part(trows(t), 0, oc)).astype(BF16)
        exchange(t, vsend.at[t], vrecv.at[t])
    gather_third(0, 1)
    gather_own(1, 1)
    gather_second(1, 1)
    gather_own(1, 0)
    gather_second(1, 0)
    gather_last(0, 1)
    for t in range(2):
        rr = pl.ds(256 * t, 256)
        vown[rr, :] = nt(hid[rr, :], W[0, g].reshape(768, 1536))
    own_heads = lanes(768 * g, 768)
    mate_heads = lanes(768 * og_, 768)
    lane = lax.broadcasted_iota(jnp.int32, (16, 128), 1)

    def row_sums(first, parts):
        acc = jnp.zeros((16, 128), F32)
        for j, v in zip(first, parts):
            acc = jnp.where(lane == j, jnp.sum(v, axis=1, keepdims=True), acc)
        return acc

    def early_sums(i, carry):
        rr = pl.ds(pl.multiple_of(16 * i, 16), 16)
        kh = (1.0 - al[...]) * hid[rr, :].astype(F32)
        mom[rr, :] = row_sums((1, 4), (kh * kh, og[rr, :].astype(F32) * kh))
        return carry

    def fwd(t):
        n = 128 * (t + 1)

        def one(h, carry):
            ATT[trows(t), lanes(768 * g + 128 * h, 128)] = nn(
                Pr[h, trows(t), pl.ds(0, n)].astype(BF16), V[pl.ds(0, n), lanes(128 * h, 128)]
            ).astype(BF16)
            return carry

        lax.fori_loop(0, 6, one, 0)

    def attn_exchange(t):
        blk = ATT.at[trows(t), own_heads]
        exchange(4 + t, blk, blk)

    for t in range(4):
        exs[t].wait()
        V[trows(t), :] = (vown[trows(t), :] + vrecv[t].astype(F32)).astype(BF16)
        fwd(t)
        if t < 2:
            attn_exchange(t)
        if t == 0:
            ins[5].wait()
            lax.fori_loop(0, 32, early_sums, 0, unroll=4)
        if t == 1:
            gather_third(1, 1, (1, 3))
        if t == 2:
            gather_third(1, 0, (1, 3))
            gather_third(1, 1, (2,))
    gather_last(1, 1)

    def late_sums(i, carry):
        rr = pl.ds(pl.multiple_of(16 * i, 16), 16)
        a = al[...]
        p = proj[rr, :]
        ap = a * p
        kh = (1.0 - a) * hid[rr, :].astype(F32)
        parts = (p * p, kh * ap, ap * ap, og[rr, :].astype(F32) * ap)
        mom[rr, :] += row_sums((0, 2, 3, 5), parts)
        return carry

    def apply(i, carry):
        rr = pl.ds(pl.multiple_of(16 * i, 16), 16)
        a = al[...]
        m = mom[rr, :]
        p = proj[rr, :]
        hf = hid[rr, :].astype(F32)
        go = og[rr, :].astype(F32)
        pr, mr, gc, pc = (m[:, j : j + 1] for j in range(4))
        mixed = hf + a * (p * pr - hf)
        og[rr, :] = (mixed * mr).astype(BF16)
        gmix = mr * (go - mixed * gc)
        proj[rr, :] = gmix * (1.0 - a)
        gpb[rr, :] = (pr * (gmix * a - p * pc)).astype(BF16)
        return carry

    def proj_own(n, carry):
        nc = lanes(384 * n, 384)
        proj[:, nc] = nn(ATT[:, own_heads], W[1, g, :, :, :, nc].reshape(768, 384))
        return carry

    def proj_more(t):
        def one(n, carry):
            nc = lanes(768 * n, 768)
            proj[trows(t), nc] += nn(ATT[trows(t), mate_heads], W[1, og_, :, :, :, nc].reshape(768, 768))
            return carry

        lax.fori_loop(0, 2, one, 0)

    def statistics(t):
        exs[4 + t].wait_recv()
        proj_more(t)
        lax.fori_loop(8 * t, 8 * t + 8, late_sums, 0, unroll=4)
        msend[t] = mom[trows(t), :].T[:8]
        rc(msend.at[t], mrecv.at[t], nm_s.at[1 + t], nm_r.at[1 + t], mate).start()

    def gradients(t):
        rc(msend.at[t], mrecv.at[t], nm_s.at[1 + t], nm_r.at[1 + t], mate).wait()
        m = [msend[t, pl.ds(j, 1), :] + mrecv[t, pl.ds(j, 1), :] for j in range(6)]
        pr = lax.rsqrt(m[0] / D + EPS)
        mr = lax.rsqrt((m[1] + 2.0 * pr * m[2] + pr * pr * m[3]) / D + EPS)
        gm = (m[4] + pr * m[5]) / D
        pm = (mr * m[5] - mr * mr * mr * gm * (m[2] + pr * m[3])) / D
        zero = jnp.zeros_like(pr)
        eight = jnp.concatenate([pr, mr, mr * mr * gm, pr * pr * pm, zero, zero, zero, zero], axis=0)
        mom[trows(t), :] = jnp.concatenate([eight, jnp.zeros((120, 128), F32)], axis=0).T
        lax.fori_loop(8 * t, 8 * t + 8, apply, 0, unroll=4)
        part = nt(gpb[trows(t), :], W[1, og_].reshape(768, 1536)).astype(BF16)
        gasend[t, 0] = part[:, :384]
        gasend[t, 1] = part[:, 384:]

    def ga_exchange(t, j):
        exchange(8 + 2 * t + j, gasend.at[t, j], garecv.at[t, j])

    lax.fori_loop(0, 4, proj_own, 0)
    gather_third(1, 0, (2,))
    gather_last(1, 0)
    statistics(0)
    attn_exchange(2)
    statistics(1)
    attn_exchange(3)
    gradients(0)
    statistics(2)
    ga_exchange(0, 0)
    ga_exchange(0, 1)
    gradients(1)
    statistics(3)
    ga_exchange(1, 0)
    gradients(2)
    ga_exchange(2, 0)
    ga_exchange(1, 1)
    rr = pl.ds(0, 256)
    vown[rr, :] = nt(gpb[rr, :], W[1, g].reshape(768, 1536))
    gradients(3)
    ga_exchange(3, 0)
    ga_exchange(2, 1)
    ga_exchange(3, 1)
    rr = pl.ds(256, 256)
    vown[rr, :] = nt(gpb[rr, :], W[1, g].reshape(768, 1536))
    for t in range(4):
        exs[4 + t].wait_send()
    outs = [pltpu.make_async_copy(og, nh_h, out_m.at[0])]
    outs[0].start()

    gsc = {}

    def half(p):
        return g if p == 0 else og_

    def rs_partner(w, p, lo, hi, left, right):
        rr = pl.ds(lo, hi - lo)
        gss[p, rr, :] = tn(
            left[:, lanes(768 * half(p) + lo, hi - lo)], right[:, lanes(768 * oc, 768)]
        ).astype(BF16)
        i = {0: 0, 384: 1, 640: 2}[lo]
        gsc[w, p, lo] = rc(gss.at[p, rr], gsr.at[w, p, rr], gs_s.at[w, p, i], gs_r.at[w, p, i], sib)
        gsc[w, p, lo].start()

    def rs_own(w, p, lo, hi, left, right):
        part = tn(left[:, lanes(768 * half(p) + lo, hi - lo)], right[:, lanes(768 * c, 768)])
        gsc[w, p, lo].wait()
        total = (part + gsr[w, p, pl.ds(lo, hi - lo), :].astype(F32)).astype(BF16)
        at = lo
        while at < hi:
            n = min(48 - at % 48, hi - at)
            b = at // 48
            RSA[w, p, b // 4, b % 4, pl.ds(at % 48, n), :] = total[at - lo : at - lo + n]
            at += n

    def rs_first(w, p):
        for d in (2, 1, 3):
            rc(
                RSA.at[w, p, :, ring(z, d), :, pl.ds(0, 384)], r1b.at[w, p, 0, d - 1],
                r1_s.at[w, p], r1_r.at[w, p, 0], zdev(d),
            ).start()
            rc(
                RSA.at[w, p, ring(y, d), :, :, pl.ds(384, 384)], r1b.at[w, p, 1, d - 1],
                r1_s.at[w, p], r1_r.at[w, p, 1], ydev(d),
            ).start()

    def rs_second(w, p):
        for s in range(2):
            rc(r1b.at[w, p, s], r1b.at[w, p, s], r1_s.at[w, p], r1_r.at[w, p, s], sib).wait_recv()
            for b in range(4):
                if s == 0:
                    acc = RSA[w, p, b, z, :, pl.ds(0, 384)].astype(F32)
                else:
                    acc = RSA[w, p, y, b, :, pl.ds(384, 384)].astype(F32)
                for d in range(3):
                    acc += r1b[w, p, s, d, b].astype(F32)
                S1[w, p, s, b] = acc.astype(BF16)
            for d in (2, 1, 3):
                at = ring(y, d) if s == 0 else ring(z, d)
                rc(
                    S1.at[w, p, s, at], r2b.at[w, p, s, d - 1],
                    r2_s.at[w, p], r2_r.at[w, p, s], ring_dev(s, True, d),
                ).start()

    def rs_third(w, p):
        for s in range(2):
            rc(r2b.at[w, p, s], r2b.at[w, p, s], r2_s.at[w, p], r2_r.at[w, p, s], sib).wait_recv()
            acc = S1[w, p, s, y if s == 0 else z].astype(F32)
            for d in range(3):
                acc += r2b[w, p, s, d].astype(F32)
            xk[w, p, :, pl.ds(384 * s, 384)] = acc

    def rs_sent(w, p):
        rc(r1b.at[w, p], r1b.at[w, p], r1_s.at[w, p], r1_r.at[w, p, 0], sib).wait_send()
        rc(r2b.at[w, p], r2b.at[w, p], r2_s.at[w, p], r2_r.at[w, p, 0], sib).wait_send()

    away = jnp.where(x == g, 1, 0)
    mine = pl.ds(pl.multiple_of(24 * c, 8), 24)
    theirs = pl.ds(pl.multiple_of(24 * oc, 8), 24)

    def owner_first(w):
        far = xk[w, away]
        near = xk[w, 1 - away]
        for i, part in enumerate((near, far)):
            dots = jnp.sum(part * U48[w, i], axis=1, keepdims=True)
            rds[w, i] = jnp.broadcast_to(dots, (48, 128))
            xs[w, i] = far[24 * i : 24 * i + 24].astype(BF16)

        def send_dots(i):
            rc(
                rds.at[w, 1 if i & 4 else 0, theirs if i & 2 else mine], rdr.at[w, i - 1],
                fd_s.at[w, 2], fd_r.at[w, 2], row(i),
            ).start()

        for i in (1, 3, 5, 7):
            send_dots(i)
        rc(xs.at[w, c], xr.at[w, 0], fd_s.at[w, 0], fd_r.at[w, 0], row(4)).start()
        rc(xs.at[w, oc], xr.at[w, 1], fd_s.at[w, 0], fd_r.at[w, 0], row(6)).start()
        rc(xk.at[w, 1 - away, theirs], gpt.at[w], fd_s.at[w, 1], fd_r.at[w, 1], sib).start()
        for i in (2, 4, 6):
            send_dots(i)

    def owner_last(w, dst, sem):
        rc(rdr.at[w], rdr.at[w], fd_s.at[w, 2], fd_r.at[w, 2], sib).wait()
        dot = rds[w, 0, mine, :]
        for i in range(7):
            dot += rdr[w, i]
        rc(gpt.at[w], gpt.at[w], fd_s.at[w, 1], fd_r.at[w, 1], sib).wait()
        rc(xr.at[w], xr.at[w], fd_s.at[w, 0], fd_r.at[w, 0], sib).wait()
        halves = (xk[w, 1 - away, mine, :] + xr[w, 0].astype(F32), gpt[w] + xr[w, 1].astype(F32))
        for at, part in zip((c, oc), halves):
            nc = lanes(768 * at, 768)
            gown[w, :, nc] = (part - unit[w, :, nc] * dot[:, :1]) / nrm[:, w : w + 1]
        cp = pltpu.make_async_copy(gown.at[w], dst, sem)
        cp.start()
        outs.append(cp)

    def bwd(h, carry):
        hc = lanes(128 * h, 128)
        for r in range(4):
            n = 128 * (r + 1)
            rr = pl.ds(128 * r, 128)
            gp = nt(GA[rr, hc], V[pl.ds(0, n), hc])
            pb = Pr[h, rr, pl.ds(0, n)]
            delta = jnp.sum(pb * gp, axis=1, keepdims=True)
            gs = (pb * (gp - delta)).astype(BF16)
            gsb[rr, pl.ds(0, n)] = gs
            gq[rr, hc] = (nn(gs, k[pl.ds(0, n), hc]) * SCALE).astype(BF16)
        gk[:, hc] = (tn(gsb[...], q[:, hc]) * SCALE).astype(BF16)
        return carry

    def value_grad(h, carry):
        hc = lanes(128 * h, 128)
        GV[:, lanes(768 * g + 128 * h, 128)] = tn(Pr[h].astype(BF16), GA[:, hc]).astype(BF16)
        return carry

    for j in range(2):
        for lo in (0, 384):
            rs_partner(1, j, lo, lo + 384, ATT, gpb)
        for lo in (0, 384):
            rs_own(1, j, lo, lo + 384, ATT, gpb)
        rs_first(1, j)
        for t in range(4):
            exs[8 + 2 * t + j].wait()
        jc = pl.ds(384 * j, 384)
        for t in range(4):
            GA[trows(t), jc] = (vown[trows(t), jc] + garecv[t, j].astype(F32)).astype(BF16)
        lax.fori_loop(3 * j, 2 * j + 3, value_grad, 0)
        blk = GV.at[:, lanes(768 * g + 384 * j, 384 - 128 * j)]
        exchange(16 + j, blk, blk)
    value_grad(5, 0)
    blk = GV.at[:, lanes(768 * g + 640, 128)]
    exchange(18, blk, blk)

    for lo in (0, 384):
        rs_partner(0, 0, lo, lo + 384, GV, hid)
    for lo in (0, 384):
        rs_own(0, 0, lo, lo + 384, GV, hid)
    rs_first(0, 0)
    lax.fori_loop(0, 2, bwd, 0)
    rs_second(1, 0)
    exs[16].wait()
    rs_partner(0, 1, 0, 384, GV, hid)
    rs_own(0, 1, 0, 384, GV, hid)
    exs[17].wait()
    rs_partner(0, 1, 384, 640, GV, hid)
    rs_own(0, 1, 384, 640, GV, hid)
    exs[18].wait()
    rs_partner(0, 1, 640, 768, GV, hid)
    rs_own(0, 1, 640, 768, GV, hid)
    rs_first(0, 1)

    def hidden_grad(n, carry):
        nc = lanes(384 * n, 384)
        gpb[:, nc] = (proj[:, nc] + nn(GV[...], W[0, :, :, :, :, nc].reshape(1536, 384))).astype(BF16)
        return carry

    lax.fori_loop(0, 4, hidden_grad, 0)
    outs.append(pltpu.make_async_copy(gpb, gh_h, out_m.at[3]))
    outs[-1].start()
    rs_second(1, 1)
    rs_second(0, 0)
    rs_third(1, 0)
    lax.fori_loop(2, 5, bwd, 0)
    rs_second(0, 1)
    rs_third(1, 1)
    owner_first(1)
    rs_third(0, 0)
    rs_third(0, 1)
    owner_first(0)
    lax.fori_loop(5, 6, bwd, 0)
    outs.append(pltpu.make_async_copy(gq, gq_h, out_m.at[1]))
    outs.append(pltpu.make_async_copy(gk, gk_h, out_m.at[2]))
    outs[-2].start()
    outs[-1].start()
    owner_last(1, gwo_h, out_m.at[4])
    owner_last(0, gwv_h, out_m.at[5])
    for w in range(2):
        for f in range(2):
            gather_sent(w, f)
            rs_sent(w, f)
    for cp in outs:
        cp.wait()


def place(*refs):
    src, dst, buf = refs[:6], refs[6:12], refs[12:18]
    sem = refs[18]
    loads = [pltpu.make_async_copy(src[i], buf[i], sem.at[0, i]) for i in range(6)]
    stores = [pltpu.make_async_copy(buf[i], dst[i], sem.at[1, i]) for i in range(6)]
    for cp in loads:
        cp.start()
    for i in range(6):
        loads[i].wait()
        stores[i].start()
    for cp in stores:
        cp.wait()


def shards(hidden, queries, attn_keys, w_value, w_out, alpha, out_grad):
    vm = pltpu.VMEM
    dma = pltpu.SemaphoreType.DMA
    hbm = pl.BlockSpec(memory_space=pltpu.HBM)
    scratch = [
        vm((1, 1536), F32), vm((512, 1536), BF16), vm((512, 768), BF16), vm((512, 768), BF16), vm((512, 1536), BF16),
        vm((2, 24, 1536), BF16), vm((2, 24, 1536), F32), vm((24, 128), F32),
        vm((8, 128), F32), vm((7, 8, 128), F32), vm((2, 3, 24, 768), BF16), vm((2, 2, 48, 768), F32),
        vm((2, 2, 4, 4, 48, 1536), BF16),
        vm((4, 128, 768), BF16), vm((4, 128, 768), BF16), vm((512, 768), F32), vm((512, 768), BF16),
        vm((6, 512, 512), F32), vm((512, 1536), BF16), vm((512, 1536), F32), vm((512, 1536), BF16),
        vm((512, 128), F32), vm((4, 8, 128), F32), vm((4, 8, 128), F32),
        vm((4, 2, 128, 384), BF16), vm((4, 2, 128, 384), BF16), vm((512, 768), BF16), vm((512, 512), BF16),
        vm((512, 768), BF16), vm((512, 768), BF16), vm((512, 1536), BF16),
        vm((2, 768, 768), BF16), vm((2, 2, 768, 768), BF16), vm((2, 2, 4, 4, 48, 768), BF16),
        vm((2, 2, 2, 3, 4, 48, 384), BF16), vm((2, 2, 2, 4, 48, 384), BF16), vm((2, 2, 2, 3, 48, 384), BF16),
        vm((2, 2, 48, 768), F32), vm((2, 2, 24, 768), BF16), vm((2, 2, 24, 768), BF16),
        vm((2, 24, 768), F32), vm((2, 24, 1536), F32), vm((2, 2, 48, 128), F32), vm((2, 7, 24, 128), F32),
        dma((6,)), dma((6,)), dma((5,)), dma((5,)), dma((2,)), dma((2,)),
        dma((2, 2)), dma((2, 2, 2, 3)), dma((2, 2)), dma((2, 2, 2, 3)), dma((2, 2)), dma((2, 2)),
        dma((19,)), dma((19,)), dma((2, 2, 3)), dma((2, 2, 3)),
        dma((2, 2)), dma((2, 2, 2)), dma((2, 2)), dma((2, 2, 2)),
        dma((2, 3)), dma((2, 3)),
    ]
    sds = jax.ShapeDtypeStruct
    shapes = (
        sds((512, 1536), BF16), sds((512, 1536), BF16), sds((512, 768), BF16),
        sds((512, 768), BF16), sds((24, 1536), F32), sds((24, 1536), F32),
    )
    made = pl.pallas_call(
        kernel,
        out_shape=shapes,
        in_specs=[hbm] * 5 + [pl.BlockSpec(memory_space=pltpu.VMEM), hbm],
        out_specs=[hbm] * 6,
        scratch_shapes=scratch,
        compiler_params=pltpu.CompilerParams(
            collective_id=0, has_side_effects=True, vmem_limit_bytes=67043328
        ),
        name="sublayer",
    )(hidden, queries, attn_keys, w_value, w_out, alpha, out_grad)
    return pl.pallas_call(
        place,
        out_shape=shapes,
        in_specs=[hbm] * 6,
        out_specs=[hbm] * 6,
        scratch_shapes=[vm(v.shape, v.dtype) for v in shapes] + [dma((2, 6))],
        name="place",
    )(*made)


def solution(mesh):
    torus = Mesh(mesh.devices.reshape(2, 4, 4, 2, mesh.shape["grp"]), AXES)
    both = P(FSDP, "grp")
    return jax.shard_map(
        shards,
        mesh=torus,
        in_specs=(both, both, both, both, both, P("grp"), both),
        out_specs=(both,) * 6,
        check_vma=False,
    )
```
